256 devices in a mesh: tx: 64 (over z, y, x_hi), ty: 2 (over x_lo), mem: 2 (over core).
Axes of the slice: x: 4 (x_hi: 2, x_lo: 2; x = x_hi * 2 + x_lo), y: 4, z: 8, core: 2. Of those that a mesh axis runs over, the one named last changes fastest.
Arguments:
- obs_value: float32 [2097152], P(('tx', 'ty', 'mem')), may hold values from -6 to 6
- obs_frac: float32 [2, 2097152], P(None, ('tx', 'ty', 'mem')), may hold values from 0 to 1
- obs_cell: int32 [2097152], P(('tx', 'ty', 'mem')), may hold values from 0 to 2047
- obs_layer: int32 [2097152], P(('tx', 'ty', 'mem')), may hold values from 0 to 11
- obs_tile: int32 [2097152], P(('tx', 'ty', 'mem')), may hold values from 0 to 127, as said below
- obs_length: int32 [256], P(('tx', 'ty', 'mem')), may hold values from 4096 to 8192, as said below
- ensemble: bfloat16 [80, 6, 2, 1024, 256], P('mem', None, None, 'tx', 'ty'), may hold values from -6 to 6
Outputs:
- alpha_grad: bfloat16 [80, 2, 1024, 256], P('mem', None, 'tx', 'ty')
The draws below stay inside these ranges and needn't reach their ends.
Inputs may be any that keep to these rules, and one draw needn't show every extreme that they name: `obs_tile`: among the 8192 entries of one device's list, padding included, at most 192 name one tile; one tile is named by exactly 192 live entries of every device's list. `obs_length`: every fourth list is full.
All inputs are finite; a program needn't handle non-finite values.
Results may differ from the reference program's by a relative error of at most 0.001.
Values sent between devices are 32-bit elements; how exact they have to be, the bound alone decides.
A program may use at most 64 MiB of HBM per device.

```python
import jax
import jax.numpy as jnp
from jax import lax

CX = 16
CY = 128
LEV = 2
SLOTS = 6
MEMBERS = 80
OBS_DEV = 8192
TILES = 128
CAP = 192
LAYERS = 12
NX = 1024
NY = 256
NSRC = 256
NOBS = 2097152
N_TY = 2


def draw_obs_tile(key, part):
    hot_tile = jax.random.randint(jax.random.fold_in(key, 11), (), 0, TILES)
    popular = jax.random.randint(jax.random.fold_in(key, 12), (TILES,), 0, 2 ** 19)
    slot_tile = jnp.arange(TILES * CAP, dtype=jnp.int32) // CAP

    def one_list(subkey):
        first_key, second_key = jax.random.split(subkey)
        score = jax.random.randint(first_key, (TILES * CAP,), 0, 2 ** 20) + popular[slot_tile]
        score = jnp.where(slot_tile == hot_tile, 2 ** 23, score)
        order = jnp.argsort(score, stable=True)
        others = slot_tile[order[:OBS_DEV - CAP]]
        front = jnp.concatenate([jnp.full((CAP,), hot_tile, jnp.int32), others[:OBS_DEV // 2 - CAP]])
        front = front[jax.random.permutation(second_key, OBS_DEV // 2)]
        return jnp.concatenate([front, others[OBS_DEV // 2 - CAP:]])
    list_keys = jax.random.split(jax.random.fold_in(key, 13), NSRC)
    return jax.vmap(one_list)(list_keys).reshape(NOBS).astype(jnp.int32)


def draw_obs_length(key, part):
    lengths = jax.random.randint(jax.random.fold_in(key, 21), (NSRC,), OBS_DEV // 2, OBS_DEV + 1)
    full_list = jnp.arange(NSRC, dtype=jnp.int32) % 4 == 0
    return jnp.where(full_list, OBS_DEV, lengths).astype(jnp.int32)


def place_ends(drawn, own_key, least, top_value):
    longest = drawn.shape.index(max(drawn.shape))
    spots = []
    for shift in (0, 1):
        where = [jax.random.randint(jax.random.fold_in(own_key, axis), (), 0, length) for axis, length in enumerate(drawn.shape)]
        where[longest] = (where[longest] + shift) % drawn.shape[longest]
        spots.append(tuple(where))
    return drawn.at[spots[0]].set(least).at[spots[1]].set(top_value)


def level_of(rng, extent, shards, low, top_value):
    loudness = 1.0
    for position, blocks in shards:
        draws = jax.random.uniform(jax.random.fold_in(jax.random.fold_in(rng, 6), position), (blocks,), jnp.float32, low / len(shards), top_value / len(shards))
        loudness = loudness * jnp.repeat(jnp.exp(draws), extent[position] // blocks).reshape((-1,) + (1,) * (len(extent) - 1 - position))
    return loudness


def normal_values(key, shape, deviation, limit, shards=(), kind=jnp.bfloat16):
    level = level_of(key, shape, shards, -0.22, 0.18) if shards else 1.0
    values = jax.random.normal(key, shape, jnp.float32) * deviation * level
    return jnp.minimum(jnp.maximum(values, -limit), limit).astype(kind)


def setup_inputs(seed: int = 0) -> dict:
    key_list = jax.random.split(jax.random.key(seed), 8)
    return {
        "obs_value": normal_values(key_list[0], (NOBS,), 1.0, 6.0, ((0, 256),), jnp.float32),
        "obs_frac": jnp.clip(1.0 * jax.random.uniform(key_list[1], (2, NOBS), jnp.float32) ** level_of(key_list[1], (2, NOBS), ((1, 256),), -0.2, 0.2), 0.0, 1.0),
        "obs_cell": place_ends(jax.random.randint(key_list[2], (NOBS,), 0, CX * CY), jax.random.fold_in(key_list[2], 1), 0, (CX * CY) - 1).astype(jnp.int32),
        "obs_layer": place_ends(jax.random.randint(key_list[3], (NOBS,), 0, LAYERS), jax.random.fold_in(key_list[3], 1), 0, LAYERS - 1).astype(jnp.int32),
        "obs_tile": draw_obs_tile(jax.random.fold_in(key_list[7], 71), 0),
        "obs_length": draw_obs_length(jax.random.fold_in(key_list[7], 71), 0),
        "ensemble": normal_values(key_list[6], (MEMBERS, SLOTS, LEV, NX, NY), 1.0, 6.0, ((0, 2), (3, 64), (4, 2))),
    }


def smooth(field):
    padded = jnp.pad(field, ((0, 0), (1, 1), (1, 1)))
    along_x = 0.25 * padded[:, :-2, :] + 0.5 * padded[:, 1:-1, :] + 0.25 * padded[:, 2:, :]
    return 0.25 * along_x[:, :, :-2] + 0.5 * along_x[:, :, 1:-1] + 0.25 * along_x[:, :, 2:]


def reference(obs_value, obs_frac, obs_cell, obs_layer, obs_tile, obs_length, ensemble):
    total = obs_value.shape[0]
    index = jnp.arange(total, dtype=jnp.int32)
    source = index // OBS_DEV
    entry = index % OBS_DEV
    live_rows = entry < obs_length[source]
    base_x = (obs_tile // N_TY) * CX + obs_cell // CY
    base_y = (obs_tile % N_TY) * CY + obs_cell % CY
    frac_x = obs_frac[0]
    frac_y = obs_frac[1]
    grad = jnp.zeros((LAYERS, NX, NY), jnp.float32)
    corners = [(0, 0, (1.0 - frac_x) * (1.0 - frac_y)), (1, 0, frac_x * (1.0 - frac_y)),
               (0, 1, (1.0 - frac_x) * frac_y), (1, 1, frac_x * frac_y)]
    for shift_x, shift_y, weight in corners:
        where_x = base_x + shift_x
        where_y = base_y + shift_y
        inside = live_rows & (where_x < NX) & (where_y < NY)
        amount = jnp.where(inside, obs_value * weight, jnp.float32(0.0))
        grad = grad.at[obs_layer, jnp.minimum(where_x, NX - 1), jnp.minimum(where_y, NY - 1)].add(amount)
    grad_slots = grad.reshape(SLOTS, LEV, NX, NY)

    def member(perturb):
        contrib = jnp.sum(perturb.astype(jnp.float32) * grad_slots, axis=0)
        return smooth(contrib).astype(jnp.bfloat16)

    return lax.map(member, ensemble)
```

```python
import functools

import jax
import jax.numpy as jnp
from jax import lax
from jax.experimental import pallas as pl
from jax.experimental.pallas import tpu as pltpu
from jax.sharding import PartitionSpec as P

F32 = jnp.float32
BF16 = jnp.bfloat16
MESH_ID = pl.DeviceIdType.MESH
VMEM_SPEC = pl.BlockSpec(memory_space=pltpu.VMEM)
SLOT = 64
TILES = 128
CHUNKS = 3
ROWS = 64
DEAD = 1000.0


def packed_iota(groups, shift):
    a = lax.broadcasted_iota(jnp.int32, (groups, 16, 128), 0)
    b = lax.broadcasted_iota(jnp.int32, (groups, 16, 128), 1)
    return (a * 16 + b + shift).astype(F32).astype(BF16)


def spread_row(row):
    return jnp.broadcast_to(row, (16, 128)).astype(BF16)[None]


def two_parts(x):
    hi = x.astype(BF16).astype(F32)
    return hi, x - hi


def dot_t(a, b):
    return lax.dot_general(a, b, (((1,), (1,)), ((), ())), preferred_element_type=F32)


def dot_n(a, b):
    return lax.dot_general(a, b, (((1,), (0,)), ((), ())), preferred_element_type=F32)


def rank_stage(length, tile_ref, d_ref, s_ref):
    i = lax.broadcasted_iota(jnp.int32, (256, 256), 0)
    j = lax.broadcasted_iota(jnp.int32, (256, 256), 1)
    before = (i < j).astype(F32).astype(BF16)
    every = jnp.ones((256, 256), BF16)
    tiles_id = lax.broadcasted_iota(jnp.int32, (TILES, 256), 0)
    lane = lax.broadcasted_iota(jnp.int32, (1, 256), 1)

    def step(k, offset):
        t = jnp.concatenate([tile_ref[pl.ds(2 * k, 1), :], tile_ref[pl.ds(2 * k + 1, 1), :]], axis=1)
        live = (lane + k * 256) < length
        t = jnp.where(live, t, -1)
        match = tiles_id == t
        hot = match.astype(F32)
        hot16 = hot.astype(BF16)
        within = dot_n(hot16, before)
        total = dot_n(hot16, every)
        rank = jnp.sum(jnp.where(match, within + offset, 0.0), axis=0, keepdims=True)
        c = jnp.floor(rank * (1.0 / SLOT))
        s = rank - c * SLOT
        d = jnp.where(live, c * TILES + t.astype(F32) - 192.0, DEAD)
        d_ref[pl.ds(2 * k, 1), :] = d[:, :128]
        d_ref[pl.ds(2 * k + 1, 1), :] = d[:, 128:]
        s_ref[pl.ds(2 * k, 1), :] = s[:, :128]
        s_ref[pl.ds(2 * k + 1, 1), :] = s[:, 128:]
        return offset + total

    lax.fori_loop(0, ROWS // 2, step, jnp.zeros((TILES, 256), F32))


def pack_stage(val_ref, frac_ref, cell_ref, layer_ref, d_ref, s_ref, acc_ref, out_ref):
    d_ids = packed_iota(24, -192)
    s_ids = packed_iota(4, 0)
    one = jnp.ones((1, 16, 128), BF16)
    zero = jnp.zeros((1, 16, 128), BF16)
    acc_ref[...] = jnp.zeros_like(acc_ref)
    per = 4

    def step(k, carry):
        lefts, highs, lows = [], [], []
        for q in range(per):
            r = k * per + q
            d = spread_row(d_ref[pl.ds(r, 1), :])
            s = spread_row(s_ref[pl.ds(r, 1), :])
            lefts.append(jnp.where(d_ids == d, one, zero).reshape(384, 128))
            mask = s_ids == s
            v = val_ref[pl.ds(r, 1), :]
            fx = frac_ref[0:1, pl.ds(pl.multiple_of(r * 128, 128), 128)]
            fy = frac_ref[1:2, pl.ds(pl.multiple_of(r * 128, 128), 128)]
            pos = layer_ref[pl.ds(r, 1), :] * 2048 + cell_ref[pl.ds(r, 1), :]
            pos_low = (pos & 255).astype(F32)
            pos_high = pos.astype(F32) - pos_low
            parts = [two_parts(v), (pos_high, pos_low), two_parts(fx), two_parts(fy)]
            for into, p in ((highs, 0), (lows, 1)):
                into.append(
                    jnp.concatenate(
                        [jnp.where(mask, spread_row(w[p]), zero).reshape(SLOT, 128) for w in parts],
                        axis=0,
                    )
                )
        left = jnp.concatenate(lefts, axis=1)
        acc_ref[...] += dot_t(left, jnp.concatenate(highs, axis=1)) + dot_t(
            left, jnp.concatenate(lows, axis=1)
        )
        return carry

    lax.fori_loop(0, ROWS // per, step, 0)
    for c in range(CHUNKS):
        for h in range(2):
            out_ref[:, 2 * c + h, :] = acc_ref[c * TILES : (c + 1) * TILES, h * 128 : (h + 1) * 128]


def pack_kernel(length_ref, val_ref, frac_ref, cell_ref, layer_ref, tile_ref, out_ref, d_ref, s_ref, acc_ref):
    rank_stage(length_ref[0], tile_ref, d_ref, s_ref)
    pack_stage(val_ref, frac_ref, cell_ref, layer_ref, d_ref, s_ref, acc_ref, out_ref)


def place_of(tx, ty):
    return tx // 8, (tx // 2) % 4, (tx % 2) * 2 + ty


def partner(tx, ty, off, sign):
    z, y, x = place_of(tx, ty)
    z = (z + sign * (off // 16) + 8) % 8
    y = (y + sign * ((off // 4) % 4) + 4) % 4
    x = (x + sign * (off % 4) + 4) % 4
    return z * 8 + y * 2 + x // 2, x % 2


def exchange_kernel(s_ref, r_ref, send_sem, recv_sem):
    tx = lax.axis_index("tx")
    ty = lax.axis_index("ty")
    me = tx * 2 + ty
    barrier = pltpu.get_barrier_semaphore()

    def greet(off, carry):
        px, py = partner(tx, ty, off, 1)
        pl.semaphore_signal(barrier, inc=1, device_id={"tx": px, "ty": py}, device_id_type=MESH_ID)
        return carry

    lax.fori_loop(1, TILES, greet, 0)
    pl.semaphore_wait(barrier, TILES - 1)

    def send(off, carry):
        px, py = partner(tx, ty, off, 1)
        pltpu.make_async_remote_copy(
            src_ref=s_ref.at[px * 2 + py],
            dst_ref=r_ref.at[me],
            send_sem=send_sem.at[off],
            recv_sem=recv_sem.at[off],
            device_id={"tx": px, "ty": py},
            device_id_type=MESH_ID,
        ).start()
        return carry

    lax.fori_loop(1, TILES, send, 0)
    r_ref[pl.ds(me, 1)] = s_ref[pl.ds(me, 1)]

    def finish(off, carry):
        px, py = partner(tx, ty, off, 1)
        qx, qy = partner(tx, ty, off, -1)
        copy = pltpu.make_async_remote_copy(
            src_ref=s_ref.at[px * 2 + py],
            dst_ref=r_ref.at[qx * 2 + qy],
            send_sem=send_sem.at[off],
            recv_sem=recv_sem.at[off],
            device_id={"tx": px, "ty": py},
            device_id_type=MESH_ID,
        )
        copy.wait_recv()
        copy.wait_send()
        return carry

    lax.fori_loop(1, TILES, finish, 0)


def spread_block(r_ref, first, acc_ref):
    lane = lax.broadcasted_iota(jnp.int32, (8, 128), 1)
    low = lane < SLOT
    x_ids = packed_iota(12, 0)
    y_ids = packed_iota(8, 0)
    rim_id = lax.broadcasted_iota(jnp.int32, (16, 128), 0)
    one = jnp.ones((1, 16, 128), BF16)
    zero = jnp.zeros((1, 16, 128), BF16)

    def both(j):
        a = r_ref[pl.ds(first, 8), j, :]
        b = r_ref[pl.ds(first + 8, 8), j, :]
        return jnp.where(low, a, pltpu.roll(b, SLOT, 1)), jnp.where(low, pltpu.roll(a, SLOT, 1), b)

    for c in range(CHUNKS):
        v, pos = both(2 * c)
        fx, fy = both(2 * c + 1)
        key = jnp.floor(pos * (1.0 / 128.0))
        cy = pos - key * 128.0
        v1 = v * fx
        v0 = v * (1.0 - fx)
        gy = 1.0 - fy
        q = [two_parts(u) for u in (v0 * gy, v0 * fy, v1 * gy, v1 * fy)]
        last = cy == 127.0
        rims = [[jnp.where(last, q[1][p], 0.0), jnp.where(last, q[3][p], 0.0)] for p in range(2)]
        rights, lefts = [], [[], []]
        for r in range(8):
            def row(u):
                return u[r : r + 1, :]
            rights.append(jnp.where(x_ids == spread_row(row(key)), one, zero).reshape(192, 128))
            here = spread_row(row(cy))
            m0 = y_ids == here
            m1 = y_ids == spread_row(row(cy) + 1.0)
            for p in range(2):
                pieces = []
                for a in range(2):
                    w0 = spread_row(row(q[2 * a][p]))
                    w1 = spread_row(row(q[2 * a + 1][p]))
                    pieces.append(jnp.where(m0, w0, jnp.where(m1, w1, zero)).reshape(128, 128))
                edge = jnp.where(
                    rim_id == 0,
                    jnp.broadcast_to(row(rims[p][0]), (16, 128)),
                    jnp.where(rim_id == 1, jnp.broadcast_to(row(rims[p][1]), (16, 128)), 0.0),
                ).astype(BF16)
                lefts[p].append(jnp.concatenate(pieces + [edge], axis=0))
        right = jnp.concatenate(rights, axis=1)
        acc_ref[...] += dot_t(jnp.concatenate(lefts[0], axis=1), right) + dot_t(
            jnp.concatenate(lefts[1], axis=1), right
        )


def spread_kernel(r_ref, base_ref, next_ref, rim_ref, acc_ref):
    acc_ref[...] = jnp.zeros_like(acc_ref)

    def step(k, carry):
        spread_block(r_ref, k * 16, acc_ref)
        return carry

    lax.fori_loop(0, 8, step, 0)
    base_ref[...] = acc_ref[0:128, :].T
    next_ref[...] = acc_ref[128:256, :].T
    rim_ref[...] = acc_ref[256:264, :]


def shifted(block, axis, distance):
    devices = range(lax.axis_size(axis))
    route = [(i - distance, i) for i in devices if i - distance in devices]
    return lax.ppermute(block, axis, route)


def of_everyone(x, axis):
    copies = jnp.broadcast_to(x, (lax.axis_size(axis), *x.shape))
    return jnp.sum(lax.all_to_all(copies, axis, split_axis=0, concat_axis=0, tiled=True), axis=0)


def extended_2(x, sides, width):
    for axis, dim in sides:
        size, length = (lax.axis_size(axis), x.shape[dim])
        up = [(i, (i + 1) % size) for i in range(size - 1)]
        down = [(j, i) for i, j in up]
        last = lax.slice_in_dim(x, length - width, length, axis=dim)
        initial = lax.slice_in_dim(x, 0, width, axis=dim)
        before = lax.ppermute(last, axis, up)
        after = lax.ppermute(initial, axis, down)
        x = jnp.concatenate([before, x, after], axis=dim)
    return x


def smooth(padded):
    along_x = 0.25 * padded[:, :, :-2, :] + 0.5 * padded[:, :, 1:-1, :] + 0.25 * padded[:, :, 2:, :]
    return 0.25 * along_x[:, :, :, :-2] + 0.5 * along_x[:, :, :, 1:-1] + 0.25 * along_x[:, :, :, 2:]


def body(obs_value, obs_frac, obs_cell, obs_layer, obs_tile, obs_length, ensemble):
    square = (ROWS, 128)
    packed = pl.pallas_call(
        pack_kernel,
        out_shape=jax.ShapeDtypeStruct((TILES, 6, 128), F32),
        in_specs=[pl.BlockSpec(memory_space=pltpu.SMEM)] + [VMEM_SPEC] * 5,
        out_specs=VMEM_SPEC,
        scratch_shapes=[pltpu.VMEM(square, F32), pltpu.VMEM(square, F32), pltpu.VMEM((384, 256), F32)],
    )(
        obs_length,
        obs_value.reshape(square),
        obs_frac,
        obs_cell.reshape(square),
        obs_layer.reshape(square),
        obs_tile.reshape(square),
    )
    got = pl.pallas_call(
        exchange_kernel,
        out_shape=jax.ShapeDtypeStruct((TILES, 6, 128), F32),
        in_specs=[VMEM_SPEC],
        out_specs=VMEM_SPEC,
        scratch_shapes=[pltpu.SemaphoreType.DMA((TILES,)), pltpu.SemaphoreType.DMA((TILES,))],
        compiler_params=pltpu.CompilerParams(collective_id=0, has_side_effects=True),
    )(packed)
    base, after, rims = pl.pallas_call(
        spread_kernel,
        out_shape=[
            jax.ShapeDtypeStruct((192, 128), F32),
            jax.ShapeDtypeStruct((192, 128), F32),
            jax.ShapeDtypeStruct((8, 192), F32),
        ],
        in_specs=[VMEM_SPEC],
        out_specs=[VMEM_SPEC] * 3,
        scratch_shapes=[pltpu.VMEM((272, 192), F32)],
    )(got)
    base = base.reshape(12, 16, 128)
    after = after.reshape(12, 16, 128)
    rim0 = rims[0].reshape(12, 16)
    rim1 = rims[1].reshape(12, 16)
    interior = base + jnp.pad(after[:, :15, :], ((0, 0), (1, 0), (0, 0)))
    east_rim = after[:, 15, :]
    north_rim = jnp.pad(rim0, ((0, 0), (0, 1))) + jnp.pad(rim1, ((0, 0), (1, 0)))
    from_south = shifted(north_rim, "ty", 1)
    interior = interior.at[:, :, 0].add(from_south[:, :16])
    east_rim = east_rim.at[:, 0].add(from_south[:, 16])
    from_west = shifted(east_rim, "tx", 1)
    interior = interior.at[:, 0, :].add(from_west)
    grad = of_everyone(interior, "mem")
    grad_slots = grad.reshape(6, 2, 16, 128)
    contrib = jnp.sum(ensemble * grad_slots[None], axis=1)
    padded = extended_2(contrib, (("tx", 2), ("ty", 3)), 1)
    return smooth(padded).astype(jnp.bfloat16)


def solution(mesh):
    placed = (
        P(("tx", "ty", "mem")),
        P(None, ("tx", "ty", "mem")),
        P(("tx", "ty", "mem")),
        P(("tx", "ty", "mem")),
        P(("tx", "ty", "mem")),
        P(("tx", "ty", "mem")),
        P("mem", None, None, "tx", "ty"),
    )
    return jax.shard_map(
        body, mesh=mesh, in_specs=placed, out_specs=P("mem", None, "tx", "ty"), check_vma=False
    )
```

```python
import functools

import jax
import jax.numpy as jnp
from jax import lax
from jax.experimental import pallas as pl
from jax.experimental.pallas import tpu as pltpu
from jax.sharding import PartitionSpec as P

F32 = jnp.float32
BF16 = jnp.bfloat16
MESH_ID = pl.DeviceIdType.MESH
VMEM_SPEC = pl.BlockSpec(memory_space=pltpu.VMEM)
SLOT = 64
TILES = 128
CHUNKS = 3
ROWS = 64
DEAD = 1000.0


def packed_iota(groups, shift):
    a = lax.broadcasted_iota(jnp.int32, (groups, 16, 128), 0)
    b = lax.broadcasted_iota(jnp.int32, (groups, 16, 128), 1)
    return (a * 16 + b + shift).astype(F32).astype(BF16)


def spread_row(row):
    return jnp.broadcast_to(row, (16, 128)).astype(BF16)[None]


def two_parts(x):
    hi = x.astype(BF16).astype(F32)
    return hi, x - hi


def dot_t(a, b):
    return lax.dot_general(a, b, (((1,), (1,)), ((), ())), preferred_element_type=F32)


def dot_n(a, b):
    return lax.dot_general(a, b, (((1,), (0,)), ((), ())), preferred_element_type=F32)


def rank_stage(length, tile_ref, d_ref, s_ref):
    i = lax.broadcasted_iota(jnp.int32, (256, 256), 0)
    j = lax.broadcasted_iota(jnp.int32, (256, 256), 1)
    before = (i < j).astype(F32).astype(BF16)
    every = jnp.ones((256, 256), BF16)
    tiles_id = lax.broadcasted_iota(jnp.int32, (TILES, 256), 0)
    lane = lax.broadcasted_iota(jnp.int32, (1, 256), 1)

    def step(k, offset):
        t = jnp.concatenate([tile_ref[pl.ds(2 * k, 1), :], tile_ref[pl.ds(2 * k + 1, 1), :]], axis=1)
        live = (lane + k * 256) < length
        t = jnp.where(live, t, -1)
        match = tiles_id == t
        hot = match.astype(F32)
        hot16 = hot.astype(BF16)
        within = dot_n(hot16, before)
        total = dot_n(hot16, every)
        rank = jnp.sum(jnp.where(match, within + offset, 0.0), axis=0, keepdims=True)
        c = jnp.floor(rank * (1.0 / SLOT))
        s = rank - c * SLOT
        d = jnp.where(live, c * TILES + t.astype(F32) - 192.0, DEAD)
        d_ref[pl.ds(2 * k, 1), :] = d[:, :128]
        d_ref[pl.ds(2 * k + 1, 1), :] = d[:, 128:]
        s_ref[pl.ds(2 * k, 1), :] = s[:, :128]
        s_ref[pl.ds(2 * k + 1, 1), :] = s[:, 128:]
        return offset + total

    lax.fori_loop(0, ROWS // 2, step, jnp.zeros((TILES, 256), F32))


def pack_stage(val_ref, frac_ref, cell_ref, layer_ref, d_ref, s_ref, acc_ref, out_ref):
    d_ids = packed_iota(24, -192)
    s_ids = packed_iota(4, 0)
    one = jnp.ones((1, 16, 128), BF16)
    zero = jnp.zeros((1, 16, 128), BF16)
    acc_ref[...] = jnp.zeros_like(acc_ref)
    per = 4

    def step(k, carry):
        lefts, highs, lows = [], [], []
        for q in range(per):
            r = k * per + q
            d = spread_row(d_ref[pl.ds(r, 1), :])
            s = spread_row(s_ref[pl.ds(r, 1), :])
            lefts.append(jnp.where(d_ids == d, one, zero).reshape(384, 128))
            mask = s_ids == s
            v = val_ref[pl.ds(r, 1), :]
            fx = frac_ref[0:1, pl.ds(pl.multiple_of(r * 128, 128), 128)]
            fy = frac_ref[1:2, pl.ds(pl.multiple_of(r * 128, 128), 128)]
            pos = layer_ref[pl.ds(r, 1), :] * 2048 + cell_ref[pl.ds(r, 1), :]
            pos_low = (pos & 255).astype(F32)
            pos_high = pos.astype(F32) - pos_low
            parts = [two_parts(v), (pos_high, pos_low), two_parts(fx), two_parts(fy)]
            for into, p in ((highs, 0), (lows, 1)):
                into.append(
                    jnp.concatenate(
                        [jnp.where(mask, spread_row(w[p]), zero).reshape(SLOT, 128) for w in parts],
                        axis=0,
                    )
                )
        left = jnp.concatenate(lefts, axis=1)
        acc_ref[...] += dot_t(left, jnp.concatenate(highs, axis=1)) + dot_t(
            left, jnp.concatenate(lows, axis=1)
        )
        return carry

    lax.fori_loop(0, ROWS // per, step, 0)
    for c in range(CHUNKS):
        for h in range(2):
            out_ref[:, 2 * c + h, :] = acc_ref[c * TILES : (c + 1) * TILES, h * 128 : (h + 1) * 128]


def place_of(tx, ty):
    return tx // 8, (tx // 2) % 4, (tx % 2) * 2 + ty


def partner(tx, ty, off, sign):
    z, y, x = place_of(tx, ty)
    z = (z + sign * (off // 16) + 8) % 8
    y = (y + sign * ((off // 4) % 4) + 4) % 4
    x = (x + sign * (off % 4) + 4) % 4
    return z * 8 + y * 2 + x // 2, x % 2


def spread_block(r_ref, first, acc_ref):
    lane = lax.broadcasted_iota(jnp.int32, (8, 128), 1)
    low = lane < SLOT
    x_ids = packed_iota(12, 0)
    y_ids = packed_iota(8, 0)
    rim_id = lax.broadcasted_iota(jnp.int32, (16, 128), 0)
    one = jnp.ones((1, 16, 128), BF16)
    zero = jnp.zeros((1, 16, 128), BF16)

    def both(j):
        a = r_ref[pl.ds(first, 8), j, :]
        b = r_ref[pl.ds(first + 8, 8), j, :]
        return jnp.where(low, a, pltpu.roll(b, SLOT, 1)), jnp.where(low, pltpu.roll(a, SLOT, 1), b)

    for c in range(CHUNKS):
        v, pos = both(2 * c)
        fx, fy = both(2 * c + 1)
        key = jnp.floor(pos * (1.0 / 128.0))
        cy = pos - key * 128.0
        v1 = v * fx
        v0 = v * (1.0 - fx)
        gy = 1.0 - fy
        q = [two_parts(u) for u in (v0 * gy, v0 * fy, v1 * gy, v1 * fy)]
        last = cy == 127.0
        rims = [[jnp.where(last, q[1][p], 0.0), jnp.where(last, q[3][p], 0.0)] for p in range(2)]
        rights, lefts = [], [[], []]
        for r in range(8):
            def row(u):
                return u[r : r + 1, :]
            rights.append(jnp.where(x_ids == spread_row(row(key)), one, zero).reshape(192, 128))
            here = spread_row(row(cy))
            m0 = y_ids == here
            m1 = y_ids == spread_row(row(cy) + 1.0)
            for p in range(2):
                pieces = []
                for a in range(2):
                    w0 = spread_row(row(q[2 * a][p]))
                    w1 = spread_row(row(q[2 * a + 1][p]))
                    pieces.append(jnp.where(m0, w0, jnp.where(m1, w1, zero)).reshape(128, 128))
                edge = jnp.where(
                    rim_id == 0,
                    jnp.broadcast_to(row(rims[p][0]), (16, 128)),
                    jnp.where(rim_id == 1, jnp.broadcast_to(row(rims[p][1]), (16, 128)), 0.0),
                ).astype(BF16)
                lefts[p].append(jnp.concatenate(pieces + [edge], axis=0))
        right = jnp.concatenate(rights, axis=1)
        acc_ref[...] += dot_t(jnp.concatenate(lefts[0], axis=1), right) + dot_t(
            jnp.concatenate(lefts[1], axis=1), right
        )


def order_of(i):
    return (i % 8) * 16 + i // 8


def remote(src, dst, send_sem, recv_sem, where):
    return pltpu.make_async_remote_copy(
        src_ref=src, dst_ref=dst, send_sem=send_sem, recv_sem=recv_sem, device_id=where, device_id_type=MESH_ID
    )


def edge_columns(ens_ref, edge, out_ref):
    k = lax.broadcasted_iota(jnp.int32, (1024, 128), 0)
    col = lax.broadcasted_iota(jnp.int32, (1024, 128), 1)
    total = jnp.zeros((192, 128), F32)
    for g in range(5):
        left = jnp.concatenate([ens_ref[8 * g + m] for m in range(8)], axis=1)
        pick = ((k % 128 == edge) & (k // 128 + 8 * g == col)).astype(F32).astype(BF16)
        total = total + dot_n(left, pick)
    out_ref[...] = total


def all_kernel(
    length_ref, val_ref, frac_ref, cell_ref, layer_ref, tile_ref, ens_hbm, out_ref,
    d_ref, s_ref, acc_ref, sbuf, rbuf, grid_ref, ens_ref, col_ref,
    part_buf, part_got, next_buf, east_buf, east_got, north_buf, north_got, corner_buf, corner_got,
    g_ref, c_ref, f_ref, xe_buf, xe_got, ce_buf, ce_got, cc_buf, cc_got, hx_ref, hy_ref,
    ens_sem, send_sem, recv_sem, send1, recv1, send2, recv2,
):
    tx = lax.axis_index("tx")
    ty = lax.axis_index("ty")
    mem = lax.axis_index("mem")
    n_tx = lax.axis_size("tx")
    east = lax.rem(tx + 1, n_tx)
    west = lax.rem(tx + n_tx - 1, n_tx)
    over = 1 - ty
    twin = 1 - mem
    barrier = pltpu.get_barrier_semaphore()

    def greet(i, carry):
        px, py = partner(tx, ty, order_of(i), 1)
        pl.semaphore_signal(barrier, inc=1, device_id={"tx": px, "ty": py, "mem": mem}, device_id_type=MESH_ID)
        return carry

    lax.fori_loop(1, TILES, greet, 0)
    for px, py in ((tx, ty), (west, ty), (tx, over), (west, over)):
        pl.semaphore_signal(barrier, inc=1, device_id={"tx": px, "ty": py, "mem": twin}, device_id_type=MESH_ID)
    ens_copy = pltpu.make_async_copy(ens_hbm, ens_ref, ens_sem)
    ens_copy.start()

    rank_stage(length_ref[0], tile_ref, d_ref, s_ref)
    pack_stage(val_ref, frac_ref, cell_ref, layer_ref, d_ref, s_ref, acc_ref, sbuf)

    pl.semaphore_wait(barrier, TILES - 1 + 4)

    def message(i):
        px, py = partner(tx, ty, order_of(i), 1)
        return remote(
            sbuf.at[px * 2 + py], rbuf.at[i], send_sem.at[i], recv_sem.at[i], {"tx": px, "ty": py, "mem": mem}
        )

    def send(i, carry):
        message(i).start()
        return carry

    lax.fori_loop(1, TILES, send, 0)
    rbuf[pl.ds(0, 1)] = sbuf[pl.ds(tx * 2 + ty, 1)]
    edge = (1 - ty) * 127
    ens_copy.wait()
    edge_columns(ens_ref, edge, col_ref)

    grid_ref[...] = jnp.zeros_like(grid_ref)

    def arrive(i, carry):
        message(i).wait_recv()
        return carry

    def gather(k, carry):
        lax.fori_loop(jnp.maximum(k * 16, 1), k * 16 + 16, arrive, 0)
        spread_block(rbuf, k * 16, grid_ref)
        return carry

    lax.fori_loop(0, 8, gather, 0)

    row = lax.broadcasted_iota(jnp.int32, (192, 128), 0)
    x_first = (row % 16) == 0
    lane192 = lax.broadcasted_iota(jnp.int32, (192, 128), 1)
    lane256 = lax.broadcasted_iota(jnp.int32, (8, 256), 1)
    row8 = lax.broadcasted_iota(jnp.int32, (8, 256), 0)
    after = grid_ref[128:256, :].T
    mine = grid_ref[0:128, :].T + jnp.where(x_first, 0.0, pltpu.roll(after, 1, 0))
    part_buf[...] = mine
    next_buf[...] = after
    east_buf[...] = next_buf[pl.ds(15, 12, stride=16), :]
    pad = jnp.zeros((8, 64), F32)
    rim0 = jnp.concatenate([jnp.broadcast_to(grid_ref[256:257, :], (8, 192)), pad], axis=1)
    rim1 = jnp.concatenate([jnp.broadcast_to(grid_ref[257:258, :], (8, 192)), pad], axis=1)
    top = row8 == 0
    first256 = (lane256 % 16) == 0
    north_buf[...] = jnp.where(top, rim0 + jnp.where(first256, 0.0, pltpu.roll(rim1, 1, 1)), 0.0)
    corner_buf[...] = jnp.where(top & first256, pltpu.roll(rim1, 241, 1), 0.0)

    first = [remote(part_buf, part_got, send1.at[0], recv1.at[0], {"tx": tx, "ty": ty, "mem": twin})]
    for j in range(2):
        first.append(remote(east_buf, east_got.at[mem], send1.at[1 + j], recv1.at[1 + mem], {"tx": east, "ty": ty, "mem": j}))
        first.append(remote(north_buf, north_got.at[mem], send1.at[3 + j], recv1.at[3 + mem], {"tx": tx, "ty": over, "mem": j}))
        first.append(remote(corner_buf, corner_got.at[mem], send1.at[5 + j], recv1.at[5 + mem], {"tx": east, "ty": over, "mem": j}))
    for copy in first:
        copy.start()
    remote(part_buf, part_got, send1.at[0], recv1.at[0], {"tx": tx, "ty": ty, "mem": twin}).wait_recv()
    for j in range(2):
        remote(east_buf, east_got.at[j], send1.at[1 + j], recv1.at[1 + j], {"tx": east, "ty": ty, "mem": j}).wait_recv()
        remote(north_buf, north_got.at[j], send1.at[3 + j], recv1.at[3 + j], {"tx": tx, "ty": over, "mem": j}).wait_recv()
        remote(corner_buf, corner_got.at[j], send1.at[5 + j], recv1.at[5 + j], {"tx": east, "ty": over, "mem": j}).wait_recv()
    has_west = jnp.where(tx > 0, 1.0, 0.0)
    has_east = jnp.where(tx < n_tx - 1, 1.0, 0.0)
    has_south = jnp.where(ty > 0, 1.0, 0.0)
    rims = (north_got[0] + north_got[1] + (corner_got[0] + corner_got[1]) * has_west) * has_south
    rims = jnp.concatenate([rims, jnp.zeros((120, 256), F32)], axis=0).T
    wall = (east_got[0] + east_got[1]) * has_west
    wall = jnp.broadcast_to(wall[:, None, :], (12, 16, 128)).reshape(192, 128)
    g = part_buf[...] + part_got[...] + rims[0:192, :] + jnp.where(x_first, wall, 0.0)
    g_ref[...] = g
    gcol = jnp.sum(jnp.where(lane192 == edge, g, 0.0), axis=1, keepdims=True)
    ce = jnp.zeros((32, 128), F32)
    for t in range(6):
        ce = ce + col_ref[t * 32 : t * 32 + 32, :] * gcol[t * 32 : t * 32 + 32, :]
    ce_buf[...] = ce
    for v in range(2):
        cc_buf[0, v : v + 1, :] = ce[v * 16 : v * 16 + 1, :]
        cc_buf[1, v : v + 1, :] = ce[v * 16 + 15 : v * 16 + 16, :]

    def contract(m, carry):
        total = jnp.zeros((32, 128), F32)
        for t in range(6):
            total = total + ens_ref[m, t * 32 : t * 32 + 32, :].astype(F32) * g_ref[t * 32 : t * 32 + 32, :]
        c_ref[pl.ds(pl.multiple_of(m * 32, 32), 32), :] = total
        return carry

    lax.fori_loop(0, 40, contract, 0)
    xe_buf[0] = c_ref[pl.ds(0, 80, stride=16), :]
    xe_buf[1] = c_ref[pl.ds(15, 80, stride=16), :]

    second = [
        remote(xe_buf.at[0], xe_got.at[1], send2.at[0], recv2.at[1], {"tx": west, "ty": ty, "mem": mem}),
        remote(xe_buf.at[1], xe_got.at[0], send2.at[1], recv2.at[0], {"tx": east, "ty": ty, "mem": mem}),
        remote(ce_buf, ce_got, send2.at[2], recv2.at[2], {"tx": tx, "ty": over, "mem": mem}),
        remote(cc_buf.at[0], cc_got.at[1], send2.at[3], recv2.at[4], {"tx": west, "ty": over, "mem": mem}),
        remote(cc_buf.at[1], cc_got.at[0], send2.at[4], recv2.at[3], {"tx": east, "ty": over, "mem": mem}),
    ]
    for copy in second:
        copy.start()

    row32 = lax.broadcasted_iota(jnp.int32, (32, 128), 0) % 16
    lane32 = lax.broadcasted_iota(jnp.int32, (32, 128), 1)

    def along_x(c):
        up = jnp.where(row32 == 0, 0.0, pltpu.roll(c, 1, 0))
        down = jnp.where(row32 == 15, 0.0, pltpu.roll(c, 31, 0))
        return 0.5 * c + 0.25 * (up + down)

    def along_y(c, lane):
        left = jnp.where(lane == 0, 0.0, pltpu.roll(c, 1, 1))
        right = jnp.where(lane == 127, 0.0, pltpu.roll(c, 127, 1))
        return 0.5 * c + 0.25 * (left + right)

    def inside(m, carry):
        at = pl.ds(pl.multiple_of(m * 32, 32), 32)
        f_ref[at, :] = along_y(along_x(c_ref[at, :]), lane32)
        return carry

    lax.fori_loop(0, 40, inside, 0)

    for copy in second:
        copy.wait_send()
    remote(xe_buf.at[0], xe_got.at[1], send2.at[0], recv2.at[1], {"tx": west, "ty": ty, "mem": mem}).wait_recv()
    remote(xe_buf.at[1], xe_got.at[0], send2.at[1], recv2.at[0], {"tx": east, "ty": ty, "mem": mem}).wait_recv()
    remote(ce_buf, ce_got, send2.at[2], recv2.at[2], {"tx": tx, "ty": over, "mem": mem}).wait_recv()
    remote(cc_buf.at[0], cc_got.at[1], send2.at[3], recv2.at[4], {"tx": west, "ty": over, "mem": mem}).wait_recv()
    remote(cc_buf.at[1], cc_got.at[0], send2.at[4], recv2.at[3], {"tx": east, "ty": over, "mem": mem}).wait_recv()

    lane80 = lax.broadcasted_iota(jnp.int32, (80, 128), 1)
    hx_ref[0] = along_y(xe_got[0], lane80) * (0.25 * has_west)
    hx_ref[1] = along_y(xe_got[1], lane80) * (0.25 * has_east)
    side = along_x(ce_got[...])
    for v in range(2):
        before = cc_got[0, v : v + 1, :] * (0.25 * has_west)
        behind = cc_got[1, v : v + 1, :] * (0.25 * has_east)
        here = lax.broadcasted_iota(jnp.int32, (32, 128), 0)
        side = side + jnp.where(here == v * 16, before, 0.0) + jnp.where(here == v * 16 + 15, behind, 0.0)
    hy_ref[...] = side * 0.25

    def finish(m, carry):
        at = pl.ds(pl.multiple_of(m * 32, 32), 32)
        f = f_ref[at, :] + jnp.where(lane32 == edge, pltpu.roll(hy_ref[...], lax.rem(edge - m + 128, 128), 1), 0.0)
        low, high = [], []
        for v in range(2):
            low.append(jnp.broadcast_to(hx_ref[0, pl.ds(2 * m + v, 1), :], (16, 128)))
            high.append(jnp.broadcast_to(hx_ref[1, pl.ds(2 * m + v, 1), :], (16, 128)))
        f = f + jnp.where(row32 == 0, jnp.concatenate(low, axis=0), 0.0)
        f = f + jnp.where(row32 == 15, jnp.concatenate(high, axis=0), 0.0)
        out_ref[m] = f.astype(BF16)
        return carry

    lax.fori_loop(0, 40, finish, 0)

    for copy in first:
        copy.wait_send()

    def sent(i, carry):
        message(i).wait_send()
        return carry

    lax.fori_loop(1, TILES, sent, 0)


def body(obs_value, obs_frac, obs_cell, obs_layer, obs_tile, obs_length, ensemble):
    square = (ROWS, 128)
    dma = pltpu.SemaphoreType.DMA
    out = pl.pallas_call(
        all_kernel,
        out_shape=jax.ShapeDtypeStruct((40, 32, 128), BF16),
        in_specs=[pl.BlockSpec(memory_space=pltpu.SMEM)] + [VMEM_SPEC] * 5 + [pl.BlockSpec(memory_space=pl.ANY)],
        out_specs=VMEM_SPEC,
        scratch_shapes=[
            pltpu.VMEM(square, F32),
            pltpu.VMEM(square, F32),
            pltpu.VMEM((384, 256), F32),
            pltpu.VMEM((TILES, 6, 128), F32),
            pltpu.VMEM((TILES, 6, 128), F32),
            pltpu.VMEM((272, 192), F32),
            pltpu.VMEM((40, 192, 128), BF16),
            pltpu.VMEM((192, 128), F32),
            pltpu.VMEM((192, 128), F32),
            pltpu.VMEM((192, 128), F32),
            pltpu.VMEM((192, 128), F32),
            pltpu.VMEM((12, 128), F32),
            pltpu.VMEM((2, 12, 128), F32),
            pltpu.VMEM((8, 256), F32),
            pltpu.VMEM((2, 8, 256), F32),
            pltpu.VMEM((8, 256), F32),
            pltpu.VMEM((2, 8, 256), F32),
            pltpu.VMEM((192, 128), F32),
            pltpu.VMEM((1280, 128), F32),
            pltpu.VMEM((1280, 128), F32),
            pltpu.VMEM((2, 80, 128), F32),
            pltpu.VMEM((2, 80, 128), F32),
            pltpu.VMEM((32, 128), F32),
            pltpu.VMEM((32, 128), F32),
            pltpu.VMEM((2, 2, 128), F32),
            pltpu.VMEM((2, 2, 128), F32),
            pltpu.VMEM((2, 80, 128), F32),
            pltpu.VMEM((32, 128), F32),
            dma,
            dma((TILES,)),
            dma((TILES,)),
            dma((7,)),
            dma((7,)),
            dma((5,)),
            dma((5,)),
        ],
        compiler_params=pltpu.CompilerParams(collective_id=0, has_side_effects=True),
    )(
        obs_length,
        obs_value.reshape(square),
        obs_frac,
        obs_cell.reshape(square),
        obs_layer.reshape(square),
        obs_tile.reshape(square),
        ensemble.reshape(40, 192, 128),
    )
    return out.reshape(40, 2, 16, 128)


def solution(mesh):
    placed = (
        P(("tx", "ty", "mem")),
        P(None, ("tx", "ty", "mem")),
        P(("tx", "ty", "mem")),
        P(("tx", "ty", "mem")),
        P(("tx", "ty", "mem")),
        P(("tx", "ty", "mem")),
        P("mem", None, None, "tx", "ty"),
    )
    return jax.shard_map(
        body, mesh=mesh, in_specs=placed, out_specs=P("mem", None, "tx", "ty"), check_vma=False
    )
```

```python
import functools

import jax
import jax.numpy as jnp
from jax import lax
from jax.experimental import pallas as pl
from jax.experimental.pallas import tpu as pltpu
from jax.sharding import PartitionSpec as P

F32 = jnp.float32
BF16 = jnp.bfloat16
MESH_ID = pl.DeviceIdType.MESH
VMEM_SPEC = pl.BlockSpec(memory_space=pltpu.VMEM)
SLOT = 64
TILES = 128
CHUNKS = 3
ROWS = 64
DEAD = 1000.0


def packed_iota(groups, shift):
    a = lax.broadcasted_iota(jnp.int32, (groups, 16, 128), 0)
    b = lax.broadcasted_iota(jnp.int32, (groups, 16, 128), 1)
    return (a * 16 + b + shift).astype(F32).astype(BF16)


def spread_row(row):
    return jnp.broadcast_to(row, (16, 128)).astype(BF16)[None]


def two_parts(x):
    hi = x.astype(BF16).astype(F32)
    return hi, x - hi


def dot_t(a, b):
    return lax.dot_general(a, b, (((1,), (1,)), ((), ())), preferred_element_type=F32)


def dot_n(a, b):
    return lax.dot_general(a, b, (((1,), (0,)), ((), ())), preferred_element_type=F32)


def rank_stage(length, tile_ref, d_ref, s_ref):
    i = lax.broadcasted_iota(jnp.int32, (128, 256), 0)
    j = lax.broadcasted_iota(jnp.int32, (128, 256), 1)
    before = jnp.where((i < j) | (j >= 128), 1.0, 0.0).astype(BF16)
    tiles_id = lax.broadcasted_iota(jnp.int32, (TILES, 128), 0)
    lane = lax.broadcasted_iota(jnp.int32, (1, 128), 1)
    per = 4

    def step(k, offset):
        for q in range(per):
            r = k * per + q
            t = tile_ref[pl.ds(r, 1), :]
            live = (lane + r * 128) < length
            t = jnp.where(live, t, -1)
            match = tiles_id == t
            both = dot_n(jnp.where(match, 1.0, 0.0).astype(BF16), before)
            rank = jnp.sum(jnp.where(match, both[:, :128] + offset, 0.0), axis=0, keepdims=True)
            offset = offset + both[:, 128:]
            c = jnp.floor(rank * (1.0 / SLOT))
            tf = t.astype(F32)
            t4 = jnp.floor(tf * 0.25)
            d_ref[pl.ds(r, 1), :] = jnp.where(live, c * 32.0 + t4, DEAD)
            s_ref[pl.ds(r, 1), :] = (tf - 4.0 * t4) * SLOT + (rank - c * SLOT)
        return offset

    lax.fori_loop(0, ROWS // per, step, jnp.zeros((TILES, 128), F32))


def pack_stage(val_ref, frac_ref, cell_ref, layer_ref, d_ref, s_ref, acc_ref, out_ref):
    d_ids = packed_iota(6, 0)
    s_ids = packed_iota(16, 0)
    one = jnp.ones((1, 16, 128), BF16)
    zero = jnp.zeros((1, 16, 128), BF16)
    acc_ref[...] = jnp.zeros_like(acc_ref)
    per = 4

    def step(k, carry):
        rights, highs, lows = [], [], []
        for q in range(per):
            r = k * per + q
            mask = d_ids == spread_row(d_ref[pl.ds(r, 1), :])
            rights.append(jnp.where(s_ids == spread_row(s_ref[pl.ds(r, 1), :]), one, zero).reshape(256, 128))
            v = val_ref[pl.ds(r, 1), :]
            fx = frac_ref[0:1, pl.ds(pl.multiple_of(r * 128, 128), 128)]
            fy = frac_ref[1:2, pl.ds(pl.multiple_of(r * 128, 128), 128)]
            pos = layer_ref[pl.ds(r, 1), :] * 2048 + cell_ref[pl.ds(r, 1), :]
            pos_low = (pos & 255).astype(F32)
            pos_high = pos.astype(F32) - pos_low
            parts = [two_parts(v), (pos_high, pos_low), two_parts(fx), two_parts(fy)]
            for into, p in ((highs, 0), (lows, 1)):
                into.append(
                    jnp.concatenate(
                        [jnp.where(mask, spread_row(w[p]), zero).reshape(96, 128) for w in parts],
                        axis=0,
                    )
                )
        right = jnp.concatenate(rights, axis=1)
        acc_ref[...] += dot_t(jnp.concatenate(highs, axis=1), right) + dot_t(
            jnp.concatenate(lows, axis=1), right
        )
        return carry

    lax.fori_loop(0, ROWS // per, step, 0)
    low = lax.broadcasted_iota(jnp.int32, (32, 128), 1) < SLOT
    for c in range(CHUNKS):
        for col in range(2):
            plain = [acc_ref[w * 96 + c * 32 : w * 96 + c * 32 + 32, col * 128 : col * 128 + 128] for w in range(4)]
            moved = [pltpu.roll(w, SLOT, 1) for w in plain]
            for half in range(2):
                at = (2 * col + half) * 32
                for h in range(2):
                    first, last = (plain[2 * h], moved[2 * h + 1]) if half == 0 else (moved[2 * h], plain[2 * h + 1])
                    out_ref[at : at + 32, 2 * c + h, :] = jnp.where(low, first, last)


def peers(tx, ty):
    z, y, x = tx // 8, (tx // 2) % 4, (tx % 2) * 2 + ty
    z_parts = [((z + dz) % 8) * 8 for dz in range(8)]

    def pair(q):
        px = (x + q) % 4
        py = (y + q // 4) % 4
        return py, px

    return z_parts, pair


def spread_block(r_ref, first, acc_ref):
    lane = lax.broadcasted_iota(jnp.int32, (8, 128), 1)
    low = lane < SLOT
    x_ids = packed_iota(12, 0)
    y_ids = packed_iota(8, 0)
    rim_id = lax.broadcasted_iota(jnp.int32, (16, 128), 0)
    one = jnp.ones((1, 16, 128), BF16)
    zero = jnp.zeros((1, 16, 128), BF16)

    def both(j):
        a = r_ref[pl.ds(first, 8), j, :]
        b = r_ref[pl.ds(first + 8, 8), j, :]
        return jnp.where(low, a, pltpu.roll(b, SLOT, 1)), jnp.where(low, pltpu.roll(a, SLOT, 1), b)

    for c in range(CHUNKS):
        v, pos = both(2 * c)
        fx, fy = both(2 * c + 1)
        key = jnp.floor(pos * (1.0 / 128.0))
        cy = pos - key * 128.0
        v1 = v * fx
        v0 = v * (1.0 - fx)
        gy = 1.0 - fy
        q = [two_parts(u) for u in (v0 * gy, v0 * fy, v1 * gy, v1 * fy)]
        last = cy == 127.0
        rims = [[jnp.where(last, q[1][p], 0.0), jnp.where(last, q[3][p], 0.0)] for p in range(2)]
        rights, lefts = [], [[], []]
        for r in range(8):
            def row(u):
                return u[r : r + 1, :]
            rights.append(jnp.where(x_ids == spread_row(row(key)), one, zero).reshape(192, 128))
            here = spread_row(row(cy))
            m0 = y_ids == here
            m1 = y_ids == spread_row(row(cy) + 1.0)
            for p in range(2):
                pieces = []
                for a in range(2):
                    w0 = spread_row(row(q[2 * a][p]))
                    w1 = spread_row(row(q[2 * a + 1][p]))
                    pieces.append(jnp.where(m0, w0, jnp.where(m1, w1, zero)).reshape(128, 128))
                edge = jnp.where(
                    rim_id == 0,
                    jnp.broadcast_to(row(rims[p][0]), (16, 128)),
                    jnp.where(rim_id == 1, jnp.broadcast_to(row(rims[p][1]), (16, 128)), 0.0),
                ).astype(BF16)
                lefts[p].append(jnp.concatenate(pieces + [edge], axis=0))
        right = jnp.concatenate(rights, axis=1)
        acc_ref[...] += dot_t(jnp.concatenate(lefts[0], axis=1), right) + dot_t(
            jnp.concatenate(lefts[1], axis=1), right
        )


def remote(src, dst, send_sem, recv_sem, where):
    return pltpu.make_async_remote_copy(
        src_ref=src, dst_ref=dst, send_sem=send_sem, recv_sem=recv_sem, device_id=where, device_id_type=MESH_ID
    )


def edge_columns(ens_ref, edge, out_ref):
    k = lax.broadcasted_iota(jnp.int32, (1024, 128), 0)
    col = lax.broadcasted_iota(jnp.int32, (1024, 128), 1)
    total = jnp.zeros((192, 128), F32)
    for g in range(5):
        left = jnp.concatenate([ens_ref[8 * g + m] for m in range(8)], axis=1)
        pick = ((k % 128 == edge) & (k // 128 + 8 * g == col)).astype(F32).astype(BF16)
        total = total + dot_n(left, pick)
    out_ref[...] = total


def all_kernel(
    length_ref, val_hbm, frac_hbm, cell_hbm, layer_hbm, tile_hbm, ens_hbm, out_ref,
    val_ref, frac_ref, cell_ref, layer_ref, tile_ref,
    d_ref, s_ref, acc_ref, sbuf, rbuf, grid_ref, ens_ref, col_ref,
    part_buf, part_got, next_buf, east_buf, east_got, north_buf, north_got, corner_buf, corner_got,
    g_ref, c_ref, f_ref, xe_buf, xe_got, ce_buf, ce_got, cc_buf, cc_got, hx_ref, hy_ref,
    in_sem, ens_sem, send_sem, recv_sem, send1, recv1, send2, recv2,
):
    tx = lax.axis_index("tx")
    ty = lax.axis_index("ty")
    mem = lax.axis_index("mem")
    n_tx = lax.axis_size("tx")
    east = lax.rem(tx + 1, n_tx)
    west = lax.rem(tx + n_tx - 1, n_tx)
    over = 1 - ty
    twin = 1 - mem
    barrier = pltpu.get_barrier_semaphore()

    z_parts, pair = peers(tx, ty)

    def over_peers(act):
        def some(q, steps):
            py, px = pair(q)
            for dz in steps:
                act(q * 8 + dz, z_parts[dz] + py * 2 + px // 2, px % 2, px * 32 + z_parts[dz] // 2 + py)

        some(0, range(1, 8))

        def step(q, carry):
            some(q, range(8))
            return carry

        lax.fori_loop(1, 16, step, 0)

    def copy_in(src, dst, i):
        copy = pltpu.make_async_copy(src, dst, in_sem.at[i])
        copy.start()
        return copy

    tile_in = copy_in(tile_hbm, tile_ref, 0)
    others_in = [
        copy_in(val_hbm, val_ref, 1),
        copy_in(frac_hbm, frac_ref, 2),
        copy_in(cell_hbm, cell_ref, 3),
        copy_in(layer_hbm, layer_ref, 4),
    ]
    ens_copy = pltpu.make_async_copy(ens_hbm, ens_ref, ens_sem)
    ens_copy.start()

    def greet(i, px, py, at):
        pl.semaphore_signal(barrier, inc=1, device_id={"tx": px, "ty": py, "mem": mem}, device_id_type=MESH_ID)

    over_peers(greet)
    for px, py in ((tx, ty), (west, ty), (tx, over), (west, over)):
        pl.semaphore_signal(barrier, inc=1, device_id={"tx": px, "ty": py, "mem": twin}, device_id_type=MESH_ID)
    tile_in.wait()
    rank_stage(length_ref[0], tile_ref, d_ref, s_ref)
    for copy in others_in:
        copy.wait()
    pack_stage(val_ref, frac_ref, cell_ref, layer_ref, d_ref, s_ref, acc_ref, sbuf)

    pl.semaphore_wait(barrier, TILES - 1 + 4)

    def message(i, px, py, at):
        return remote(sbuf.at[at], rbuf.at[i], send_sem.at[i], recv_sem.at[i], {"tx": px, "ty": py, "mem": mem})

    def slot(i):
        return message(i, west, ty, 0)

    over_peers(lambda *peer: message(*peer).start())
    z_own, pair_own = z_parts[0], pair(0)
    rbuf[pl.ds(0, 1)] = sbuf[pl.ds(pair_own[1] * 32 + z_own // 2 + pair_own[0], 1)]
    edge = (1 - ty) * 127
    ens_copy.wait()
    edge_columns(ens_ref, edge, col_ref)

    grid_ref[...] = jnp.zeros_like(grid_ref)

    def arrive(i, carry):
        slot(i).wait_recv()
        return carry

    def gather(k, carry):
        lax.fori_loop(jnp.maximum(k * 16, 1), k * 16 + 16, arrive, 0)
        spread_block(rbuf, k * 16, grid_ref)
        return carry

    lax.fori_loop(0, 8, gather, 0)

    row = lax.broadcasted_iota(jnp.int32, (192, 128), 0)
    x_first = (row % 16) == 0
    lane192 = lax.broadcasted_iota(jnp.int32, (192, 128), 1)
    lane256 = lax.broadcasted_iota(jnp.int32, (8, 256), 1)
    row8 = lax.broadcasted_iota(jnp.int32, (8, 256), 0)
    after = grid_ref[128:256, :].T
    mine = grid_ref[0:128, :].T + jnp.where(x_first, 0.0, pltpu.roll(after, 1, 0))
    part_buf[...] = mine
    next_buf[...] = after
    east_buf[...] = next_buf[pl.ds(15, 12, stride=16), :]
    pad = jnp.zeros((8, 64), F32)
    rim0 = jnp.concatenate([jnp.broadcast_to(grid_ref[256:257, :], (8, 192)), pad], axis=1)
    rim1 = jnp.concatenate([jnp.broadcast_to(grid_ref[257:258, :], (8, 192)), pad], axis=1)
    top = row8 == 0
    first256 = (lane256 % 16) == 0
    north_buf[...] = jnp.where(top, rim0 + jnp.where(first256, 0.0, pltpu.roll(rim1, 1, 1)), 0.0)
    corner_buf[...] = jnp.where(top & first256, pltpu.roll(rim1, 241, 1), 0.0)

    first = [remote(part_buf, part_got, send1.at[0], recv1.at[0], {"tx": tx, "ty": ty, "mem": twin})]
    for j in range(2):
        first.append(remote(east_buf, east_got.at[mem], send1.at[1 + j], recv1.at[1 + mem], {"tx": east, "ty": ty, "mem": j}))
        first.append(remote(north_buf, north_got.at[mem], send1.at[3 + j], recv1.at[3 + mem], {"tx": tx, "ty": over, "mem": j}))
        first.append(remote(corner_buf, corner_got.at[mem], send1.at[5 + j], recv1.at[5 + mem], {"tx": east, "ty": over, "mem": j}))
    for copy in first:
        copy.start()
    remote(part_buf, part_got, send1.at[0], recv1.at[0], {"tx": tx, "ty": ty, "mem": twin}).wait_recv()
    for j in range(2):
        remote(east_buf, east_got.at[j], send1.at[1 + j], recv1.at[1 + j], {"tx": east, "ty": ty, "mem": j}).wait_recv()
        remote(north_buf, north_got.at[j], send1.at[3 + j], recv1.at[3 + j], {"tx": tx, "ty": over, "mem": j}).wait_recv()
        remote(corner_buf, corner_got.at[j], send1.at[5 + j], recv1.at[5 + j], {"tx": east, "ty": over, "mem": j}).wait_recv()
    has_west = jnp.where(tx > 0, 1.0, 0.0)
    has_east = jnp.where(tx < n_tx - 1, 1.0, 0.0)
    has_south = jnp.where(ty > 0, 1.0, 0.0)
    rims = (north_got[0] + north_got[1] + (corner_got[0] + corner_got[1]) * has_west) * has_south
    rims = jnp.concatenate([rims, jnp.zeros((120, 256), F32)], axis=0).T
    wall = (east_got[0] + east_got[1]) * has_west
    wall = jnp.broadcast_to(wall[:, None, :], (12, 16, 128)).reshape(192, 128)
    g = part_buf[...] + part_got[...] + rims[0:192, :] + jnp.where(x_first, wall, 0.0)
    g_ref[...] = g
    gcol = jnp.sum(jnp.where(lane192 == edge, g, 0.0), axis=1, keepdims=True)
    ce = jnp.zeros((32, 128), F32)
    for t in range(6):
        ce = ce + col_ref[t * 32 : t * 32 + 32, :] * gcol[t * 32 : t * 32 + 32, :]
    ce_buf[...] = ce
    for v in range(2):
        cc_buf[0, v : v + 1, :] = ce[v * 16 : v * 16 + 1, :]
        cc_buf[1, v : v + 1, :] = ce[v * 16 + 15 : v * 16 + 16, :]

    def contract(m, carry):
        total = jnp.zeros((32, 128), F32)
        for t in range(6):
            total = total + ens_ref[m, t * 32 : t * 32 + 32, :].astype(F32) * g_ref[t * 32 : t * 32 + 32, :]
        c_ref[pl.ds(pl.multiple_of(m * 32, 32), 32), :] = total
        return carry

    lax.fori_loop(0, 40, contract, 0)
    xe_buf[0] = c_ref[pl.ds(0, 80, stride=16), :]
    xe_buf[1] = c_ref[pl.ds(15, 80, stride=16), :]

    second = [
        remote(xe_buf.at[0], xe_got.at[1], send2.at[0], recv2.at[1], {"tx": west, "ty": ty, "mem": mem}),
        remote(xe_buf.at[1], xe_got.at[0], send2.at[1], recv2.at[0], {"tx": east, "ty": ty, "mem": mem}),
        remote(ce_buf, ce_got, send2.at[2], recv2.at[2], {"tx": tx, "ty": over, "mem": mem}),
        remote(cc_buf.at[0], cc_got.at[1], send2.at[3], recv2.at[4], {"tx": west, "ty": over, "mem": mem}),
        remote(cc_buf.at[1], cc_got.at[0], send2.at[4], recv2.at[3], {"tx": east, "ty": over, "mem": mem}),
    ]
    for copy in second:
        copy.start()

    row32 = lax.broadcasted_iota(jnp.int32, (32, 128), 0) % 16
    lane32 = lax.broadcasted_iota(jnp.int32, (32, 128), 1)

    def along_x(c):
        up = jnp.where(row32 == 0, 0.0, pltpu.roll(c, 1, 0))
        down = jnp.where(row32 == 15, 0.0, pltpu.roll(c, 31, 0))
        return 0.5 * c + 0.25 * (up + down)

    def along_y(c, lane):
        left = jnp.where(lane == 0, 0.0, pltpu.roll(c, 1, 1))
        right = jnp.where(lane == 127, 0.0, pltpu.roll(c, 127, 1))
        return 0.5 * c + 0.25 * (left + right)

    def inside(m, carry):
        at = pl.ds(pl.multiple_of(m * 32, 32), 32)
        f_ref[at, :] = along_y(along_x(c_ref[at, :]), lane32)
        return carry

    lax.fori_loop(0, 40, inside, 0)

    for copy in second:
        copy.wait_send()
    remote(xe_buf.at[0], xe_got.at[1], send2.at[0], recv2.at[1], {"tx": west, "ty": ty, "mem": mem}).wait_recv()
    remote(xe_buf.at[1], xe_got.at[0], send2.at[1], recv2.at[0], {"tx": east, "ty": ty, "mem": mem}).wait_recv()
    remote(ce_buf, ce_got, send2.at[2], recv2.at[2], {"tx": tx, "ty": over, "mem": mem}).wait_recv()
    remote(cc_buf.at[0], cc_got.at[1], send2.at[3], recv2.at[4], {"tx": west, "ty": over, "mem": mem}).wait_recv()
    remote(cc_buf.at[1], cc_got.at[0], send2.at[4], recv2.at[3], {"tx": east, "ty": over, "mem": mem}).wait_recv()

    lane80 = lax.broadcasted_iota(jnp.int32, (80, 128), 1)
    hx_ref[0] = along_y(xe_got[0], lane80) * (0.25 * has_west)
    hx_ref[1] = along_y(xe_got[1], lane80) * (0.25 * has_east)
    side = along_x(ce_got[...])
    for v in range(2):
        before = cc_got[0, v : v + 1, :] * (0.25 * has_west)
        behind = cc_got[1, v : v + 1, :] * (0.25 * has_east)
        here = lax.broadcasted_iota(jnp.int32, (32, 128), 0)
        side = side + jnp.where(here == v * 16, before, 0.0) + jnp.where(here == v * 16 + 15, behind, 0.0)
    hy_ref[...] = side * 0.25

    def finish(m, carry):
        at = pl.ds(pl.multiple_of(m * 32, 32), 32)
        f = f_ref[at, :] + jnp.where(lane32 == edge, pltpu.roll(hy_ref[...], lax.rem(edge - m + 128, 128), 1), 0.0)
        low, high = [], []
        for v in range(2):
            low.append(jnp.broadcast_to(hx_ref[0, pl.ds(2 * m + v, 1), :], (16, 128)))
            high.append(jnp.broadcast_to(hx_ref[1, pl.ds(2 * m + v, 1), :], (16, 128)))
        f = f + jnp.where(row32 == 0, jnp.concatenate(low, axis=0), 0.0)
        f = f + jnp.where(row32 == 15, jnp.concatenate(high, axis=0), 0.0)
        out_ref[m] = f.astype(BF16)
        return carry

    lax.fori_loop(0, 40, finish, 0)

    for copy in first:
        copy.wait_send()

    def sent(i, carry):
        slot(i).wait_send()
        return carry

    lax.fori_loop(1, TILES, sent, 0)


def body(obs_value, obs_frac, obs_cell, obs_layer, obs_tile, obs_length, ensemble):
    square = (ROWS, 128)
    dma = pltpu.SemaphoreType.DMA
    out = pl.pallas_call(
        all_kernel,
        out_shape=jax.ShapeDtypeStruct((40, 32, 128), BF16),
        in_specs=[pl.BlockSpec(memory_space=pltpu.SMEM)] + [pl.BlockSpec(memory_space=pl.ANY)] * 6,
        out_specs=VMEM_SPEC,
        scratch_shapes=[
            pltpu.VMEM(square, F32),
            pltpu.VMEM((2, ROWS * 128), F32),
            pltpu.VMEM(square, jnp.int32),
            pltpu.VMEM(square, jnp.int32),
            pltpu.VMEM(square, jnp.int32),
            pltpu.VMEM(square, F32),
            pltpu.VMEM(square, F32),
            pltpu.VMEM((384, 256), F32),
            pltpu.VMEM((TILES, 6, 128), F32),
            pltpu.VMEM((TILES, 6, 128), F32),
            pltpu.VMEM((272, 192), F32),
            pltpu.VMEM((40, 192, 128), BF16),
            pltpu.VMEM((192, 128), F32),
            pltpu.VMEM((192, 128), F32),
            pltpu.VMEM((192, 128), F32),
            pltpu.VMEM((192, 128), F32),
            pltpu.VMEM((12, 128), F32),
            pltpu.VMEM((2, 12, 128), F32),
            pltpu.VMEM((8, 256), F32),
            pltpu.VMEM((2, 8, 256), F32),
            pltpu.VMEM((8, 256), F32),
            pltpu.VMEM((2, 8, 256), F32),
            pltpu.VMEM((192, 128), F32),
            pltpu.VMEM((1280, 128), F32),
            pltpu.VMEM((1280, 128), F32),
            pltpu.VMEM((2, 80, 128), F32),
            pltpu.VMEM((2, 80, 128), F32),
            pltpu.VMEM((32, 128), F32),
            pltpu.VMEM((32, 128), F32),
            pltpu.VMEM((2, 2, 128), F32),
            pltpu.VMEM((2, 2, 128), F32),
            pltpu.VMEM((2, 80, 128), F32),
            pltpu.VMEM((32, 128), F32),
            dma((5,)),
            dma,
            dma((TILES,)),
            dma((TILES,)),
            dma((7,)),
            dma((7,)),
            dma((5,)),
            dma((5,)),
        ],
        compiler_params=pltpu.CompilerParams(collective_id=0, has_side_effects=True),
    )(
        obs_length,
        obs_value.reshape(square),
        obs_frac,
        obs_cell.reshape(square),
        obs_layer.reshape(square),
        obs_tile.reshape(square),
        ensemble.reshape(40, 192, 128),
    )
    return out.reshape(40, 2, 16, 128)


def solution(mesh):
    placed = (
        P(("tx", "ty", "mem")),
        P(None, ("tx", "ty", "mem")),
        P(("tx", "ty", "mem")),
        P(("tx", "ty", "mem")),
        P(("tx", "ty", "mem")),
        P(("tx", "ty", "mem")),
        P("mem", None, None, "tx", "ty"),
    )
    return jax.shard_map(
        body, mesh=mesh, in_specs=placed, out_specs=P("mem", None, "tx", "ty"), check_vma=False
    )
```

```python
import functools

import jax
import jax.numpy as jnp
from jax import lax
from jax.experimental import pallas as pl
from jax.experimental.pallas import tpu as pltpu
from jax.sharding import PartitionSpec as P

F32 = jnp.float32
BF16 = jnp.bfloat16
MESH_ID = pl.DeviceIdType.MESH
VMEM_SPEC = pl.BlockSpec(memory_space=pltpu.VMEM)
SLOT = 64
TILES = 128
CHUNKS = 3
ROWS = 64
DEAD = 1000.0


def packed_iota(groups, shift):
    a = lax.broadcasted_iota(jnp.int32, (groups, 16, 128), 0)
    b = lax.broadcasted_iota(jnp.int32, (groups, 16, 128), 1)
    return (a * 16 + b + shift).astype(F32).astype(BF16)


def spread_row(row):
    return jnp.broadcast_to(row, (16, 128)).astype(BF16)[None]


def two_parts(x):
    hi = x.astype(BF16).astype(F32)
    return hi, x - hi


def dot_t(a, b):
    return lax.dot_general(a, b, (((1,), (1,)), ((), ())), preferred_element_type=F32)


def dot_n(a, b):
    return lax.dot_general(a, b, (((1,), (0,)), ((), ())), preferred_element_type=F32)


def rank_stage(length, tile_ref, d_ref, s_ref):
    i = lax.broadcasted_iota(jnp.int32, (128, 256), 0)
    j = lax.broadcasted_iota(jnp.int32, (128, 256), 1)
    before = jnp.where((i < j) | (j >= 128), 1.0, 0.0).astype(BF16)
    tiles_id = lax.broadcasted_iota(jnp.int32, (TILES, 128), 0)
    lane = lax.broadcasted_iota(jnp.int32, (1, 128), 1)
    per = 4

    def step(k, offset):
        for q in range(per):
            r = k * per + q
            t = tile_ref[pl.ds(r, 1), :]
            live = (lane + r * 128) < length
            t = jnp.where(live, t, -1)
            match = tiles_id == t
            both = dot_n(jnp.where(match, 1.0, 0.0).astype(BF16), before)
            rank = jnp.sum(jnp.where(match, both[:, :128] + offset, 0.0), axis=0, keepdims=True)
            offset = offset + both[:, 128:]
            c = jnp.floor(rank * (1.0 / SLOT))
            tf = t.astype(F32)
            t4 = jnp.floor(tf * 0.25)
            d_ref[pl.ds(r, 1), :] = jnp.where(live, c * 32.0 + t4, DEAD)
            s_ref[pl.ds(r, 1), :] = (tf - 4.0 * t4) * SLOT + (rank - c * SLOT)
        return offset

    lax.fori_loop(0, ROWS // per, step, jnp.zeros((TILES, 128), F32))


def pack_stage(val_ref, frac_ref, cell_ref, layer_ref, d_ref, s_ref, acc_ref, out_ref):
    d_ids = packed_iota(6, 0)
    s_ids = packed_iota(16, 0)
    one = jnp.ones((1, 16, 128), BF16)
    zero = jnp.zeros((1, 16, 128), BF16)
    acc_ref[...] = jnp.zeros_like(acc_ref)
    per = 16

    def step(k, carry):
        rights, highs, lows = [], [], []
        for q in range(per):
            r = k * per + q
            mask = d_ids == spread_row(d_ref[pl.ds(r, 1), :])
            rights.append(jnp.where(s_ids == spread_row(s_ref[pl.ds(r, 1), :]), one, zero).reshape(256, 128))
            v = val_ref[pl.ds(r, 1), :]
            fx = frac_ref[0:1, pl.ds(pl.multiple_of(r * 128, 128), 128)]
            fy = frac_ref[1:2, pl.ds(pl.multiple_of(r * 128, 128), 128)]
            pos = layer_ref[pl.ds(r, 1), :] * 2048 + cell_ref[pl.ds(r, 1), :]
            pos_low = (pos & 255).astype(F32)
            pos_high = pos.astype(F32) - pos_low
            parts = [two_parts(v), (pos_high, pos_low), two_parts(fx), two_parts(fy)]
            for into, p in ((highs, 0), (lows, 1)):
                into.append(
                    jnp.concatenate(
                        [jnp.where(mask, spread_row(w[p]), zero).reshape(96, 128) for w in parts],
                        axis=0,
                    )
                )
        right = jnp.concatenate(rights, axis=1)
        acc_ref[...] += dot_t(jnp.concatenate(highs, axis=1), right) + dot_t(
            jnp.concatenate(lows, axis=1), right
        )
        return carry

    lax.fori_loop(0, ROWS // per, step, 0)
    low = lax.broadcasted_iota(jnp.int32, (32, 128), 1) < SLOT
    for c in range(CHUNKS):
        for col in range(2):
            plain = [acc_ref[w * 96 + c * 32 : w * 96 + c * 32 + 32, col * 128 : col * 128 + 128] for w in range(4)]
            moved = [pltpu.roll(w, SLOT, 1) for w in plain]
            for half in range(2):
                at = (2 * col + half) * 32
                for h in range(2):
                    first, last = (plain[2 * h], moved[2 * h + 1]) if half == 0 else (moved[2 * h], plain[2 * h + 1])
                    out_ref[at : at + 32, 2 * c + h, :] = jnp.where(low, first, last)


def peers(tx, ty):
    z, y, x = tx // 8, (tx // 2) % 4, (tx % 2) * 2 + ty
    z_parts = [((z + dz) % 8) * 8 for dz in range(8)]

    def pair(q):
        px = (x + q) % 4
        py = (y + q // 4) % 4
        return py, px

    return z_parts, pair


def spread_block(r_ref, first, acc_ref):
    lane = lax.broadcasted_iota(jnp.int32, (8, 128), 1)
    low = lane < SLOT
    x_ids = packed_iota(12, 0)
    y_ids = packed_iota(8, 0)
    rim_id = lax.broadcasted_iota(jnp.int32, (16, 128), 0)
    one = jnp.ones((1, 16, 128), BF16)
    zero = jnp.zeros((1, 16, 128), BF16)

    def both(j):
        a = r_ref[pl.ds(first, 8), j, :]
        b = r_ref[pl.ds(first + 8, 8), j, :]
        return jnp.where(low, a, pltpu.roll(b, SLOT, 1)), jnp.where(low, pltpu.roll(a, SLOT, 1), b)

    for c in range(CHUNKS):
        v, pos = both(2 * c)
        fx, fy = both(2 * c + 1)
        key = jnp.floor(pos * (1.0 / 128.0))
        cy = pos - key * 128.0
        v1 = v * fx
        v0 = v * (1.0 - fx)
        gy = 1.0 - fy
        q = [two_parts(u) for u in (v0 * gy, v0 * fy, v1 * gy, v1 * fy)]
        last = cy == 127.0
        rims = [[jnp.where(last, q[1][p], 0.0), jnp.where(last, q[3][p], 0.0)] for p in range(2)]
        rights, lefts = [], [[], []]
        for r in range(8):
            def row(u):
                return u[r : r + 1, :]
            rights.append(jnp.where(x_ids == spread_row(row(key)), one, zero).reshape(192, 128))
            here = spread_row(row(cy))
            m0 = y_ids == here
            m1 = y_ids == spread_row(row(cy) + 1.0)
            for p in range(2):
                pieces = []
                for a in range(2):
                    w0 = spread_row(row(q[2 * a][p]))
                    w1 = spread_row(row(q[2 * a + 1][p]))
                    pieces.append(jnp.where(m0, w0, jnp.where(m1, w1, zero)).reshape(128, 128))
                edge = jnp.where(
                    rim_id == 0,
                    jnp.broadcast_to(row(rims[p][0]), (16, 128)),
                    jnp.where(rim_id == 1, jnp.broadcast_to(row(rims[p][1]), (16, 128)), 0.0),
                ).astype(BF16)
                lefts[p].append(jnp.concatenate(pieces + [edge], axis=0))
        right = jnp.concatenate(rights, axis=1)
        acc_ref[...] += dot_t(jnp.concatenate(lefts[0], axis=1), right) + dot_t(
            jnp.concatenate(lefts[1], axis=1), right
        )


def remote(src, dst, send_sem, recv_sem, where):
    return pltpu.make_async_remote_copy(
        src_ref=src, dst_ref=dst, send_sem=send_sem, recv_sem=recv_sem, device_id=where, device_id_type=MESH_ID
    )


def edge_columns(ens_ref, edge, out_ref):
    k = lax.broadcasted_iota(jnp.int32, (1024, 128), 0)
    col = lax.broadcasted_iota(jnp.int32, (1024, 128), 1)
    total = jnp.zeros((192, 128), F32)
    for g in range(5):
        left = jnp.concatenate([ens_ref[8 * g + m] for m in range(8)], axis=1)
        pick = ((k % 128 == edge) & (k // 128 + 8 * g == col)).astype(F32).astype(BF16)
        total = total + dot_n(left, pick)
    out_ref[...] = total


def all_kernel(
    length_ref, val_hbm, frac_hbm, cell_hbm, layer_hbm, tile_hbm, ens_hbm, out_ref,
    val_ref, frac_ref, cell_ref, layer_ref, tile_ref,
    d_ref, s_ref, acc_ref, sbuf, rbuf, grid_ref, ens_ref, col_ref,
    part_buf, part_got, next_buf, east_buf, east_got, north_buf, north_got, corner_buf, corner_got,
    g_ref, c_ref, f_ref, xe_buf, xe_got, ce_buf, ce_got, cc_buf, cc_got, hx_ref, hy_ref,
    in_sem, ens_sem, send_sem, recv_sem, send1, recv1, send2, recv2,
):
    tx = lax.axis_index("tx")
    ty = lax.axis_index("ty")
    mem = lax.axis_index("mem")
    n_tx = lax.axis_size("tx")
    east = lax.rem(tx + 1, n_tx)
    west = lax.rem(tx + n_tx - 1, n_tx)
    over = 1 - ty
    twin = 1 - mem
    barrier = pltpu.get_barrier_semaphore()

    z_parts, pair = peers(tx, ty)

    def over_peers(act):
        def some(q, steps):
            py, px = pair(q)
            for dz in steps:
                act(q * 8 + dz, z_parts[dz] + py * 2 + px // 2, px % 2, px * 32 + z_parts[dz] // 2 + py)

        some(0, range(1, 8))

        def step(q, carry):
            some(q, range(8))
            return carry

        lax.fori_loop(1, 16, step, 0)

    def copy_in(src, dst, i):
        copy = pltpu.make_async_copy(src, dst, in_sem.at[i])
        copy.start()
        return copy

    tile_in = copy_in(tile_hbm, tile_ref, 0)
    others_in = [
        copy_in(val_hbm, val_ref, 1),
        copy_in(frac_hbm, frac_ref, 2),
        copy_in(cell_hbm, cell_ref, 3),
        copy_in(layer_hbm, layer_ref, 4),
    ]
    ens_copy = pltpu.make_async_copy(ens_hbm, ens_ref, ens_sem)
    ens_copy.start()

    def greet(i, px, py, at):
        pl.semaphore_signal(barrier, inc=1, device_id={"tx": px, "ty": py, "mem": mem}, device_id_type=MESH_ID)

    over_peers(greet)
    for px, py in ((tx, ty), (west, ty), (tx, over), (west, over)):
        pl.semaphore_signal(barrier, inc=1, device_id={"tx": px, "ty": py, "mem": twin}, device_id_type=MESH_ID)
    tile_in.wait()
    rank_stage(length_ref[0], tile_ref, d_ref, s_ref)
    for copy in others_in:
        copy.wait()
    pack_stage(val_ref, frac_ref, cell_ref, layer_ref, d_ref, s_ref, acc_ref, sbuf)

    pl.semaphore_wait(barrier, TILES - 1 + 4)

    def message(i, px, py, at):
        return remote(sbuf.at[at], rbuf.at[i], send_sem, recv_sem.at[i // 16], {"tx": px, "ty": py, "mem": mem})

    def group(k, first, count):
        at = pl.ds(first, count)
        return remote(sbuf.at[at], rbuf.at[at], send_sem, recv_sem.at[k], {"tx": west, "ty": ty, "mem": mem})

    over_peers(lambda *peer: message(*peer).start())
    z_own, pair_own = z_parts[0], pair(0)
    rbuf[pl.ds(0, 1)] = sbuf[pl.ds(pair_own[1] * 32 + z_own // 2 + pair_own[0], 1)]
    edge = (1 - ty) * 127
    ens_copy.wait()
    edge_columns(ens_ref, edge, col_ref)

    grid_ref[...] = jnp.zeros_like(grid_ref)

    group(0, 1, 15).wait_recv()
    spread_block(rbuf, 0, grid_ref)

    def gather(k, carry):
        group(k, k * 16, 16).wait_recv()
        spread_block(rbuf, k * 16, grid_ref)
        return carry

    lax.fori_loop(1, 8, gather, 0)

    row = lax.broadcasted_iota(jnp.int32, (192, 128), 0)
    x_first = (row % 16) == 0
    lane192 = lax.broadcasted_iota(jnp.int32, (192, 128), 1)
    lane256 = lax.broadcasted_iota(jnp.int32, (8, 256), 1)
    row8 = lax.broadcasted_iota(jnp.int32, (8, 256), 0)
    after = grid_ref[128:256, :].T
    mine = grid_ref[0:128, :].T + jnp.where(x_first, 0.0, pltpu.roll(after, 1, 0))
    part_buf[...] = mine
    next_buf[...] = after
    east_buf[...] = next_buf[pl.ds(15, 12, stride=16), :]
    pad = jnp.zeros((8, 64), F32)
    rim0 = jnp.concatenate([jnp.broadcast_to(grid_ref[256:257, :], (8, 192)), pad], axis=1)
    rim1 = jnp.concatenate([jnp.broadcast_to(grid_ref[257:258, :], (8, 192)), pad], axis=1)
    top = row8 == 0
    first256 = (lane256 % 16) == 0
    north_buf[...] = jnp.where(top, rim0 + jnp.where(first256, 0.0, pltpu.roll(rim1, 1, 1)), 0.0)
    corner_buf[...] = jnp.where(top & first256, pltpu.roll(rim1, 241, 1), 0.0)

    first = [remote(part_buf, part_got, send1.at[0], recv1.at[0], {"tx": tx, "ty": ty, "mem": twin})]
    for j in range(2):
        first.append(remote(east_buf, east_got.at[mem], send1.at[1 + j], recv1.at[1 + mem], {"tx": east, "ty": ty, "mem": j}))
        first.append(remote(north_buf, north_got.at[mem], send1.at[3 + j], recv1.at[3 + mem], {"tx": tx, "ty": over, "mem": j}))
        first.append(remote(corner_buf, corner_got.at[mem], send1.at[5 + j], recv1.at[5 + mem], {"tx": east, "ty": over, "mem": j}))
    for copy in first:
        copy.start()
    remote(part_buf, part_got, send1.at[0], recv1.at[0], {"tx": tx, "ty": ty, "mem": twin}).wait_recv()
    for j in range(2):
        remote(east_buf, east_got.at[j], send1.at[1 + j], recv1.at[1 + j], {"tx": east, "ty": ty, "mem": j}).wait_recv()
        remote(north_buf, north_got.at[j], send1.at[3 + j], recv1.at[3 + j], {"tx": tx, "ty": over, "mem": j}).wait_recv()
        remote(corner_buf, corner_got.at[j], send1.at[5 + j], recv1.at[5 + j], {"tx": east, "ty": over, "mem": j}).wait_recv()
    has_west = jnp.where(tx > 0, 1.0, 0.0)
    has_east = jnp.where(tx < n_tx - 1, 1.0, 0.0)
    has_south = jnp.where(ty > 0, 1.0, 0.0)
    rims = (north_got[0] + north_got[1] + (corner_got[0] + corner_got[1]) * has_west) * has_south
    rims = jnp.concatenate([rims, jnp.zeros((120, 256), F32)], axis=0).T
    wall = (east_got[0] + east_got[1]) * has_west
    wall = jnp.broadcast_to(wall[:, None, :], (12, 16, 128)).reshape(192, 128)
    g = part_buf[...] + part_got[...] + rims[0:192, :] + jnp.where(x_first, wall, 0.0)
    g_ref[...] = g
    gcol = jnp.sum(jnp.where(lane192 == edge, g, 0.0), axis=1, keepdims=True)
    ce = jnp.zeros((32, 128), F32)
    for t in range(6):
        ce = ce + col_ref[t * 32 : t * 32 + 32, :] * gcol[t * 32 : t * 32 + 32, :]
    ce_buf[...] = ce
    for v in range(2):
        cc_buf[0, v : v + 1, :] = ce[v * 16 : v * 16 + 1, :]
        cc_buf[1, v : v + 1, :] = ce[v * 16 + 15 : v * 16 + 16, :]

    def contract(m, carry):
        total = jnp.zeros((32, 128), F32)
        for t in range(6):
            total = total + ens_ref[m, t * 32 : t * 32 + 32, :].astype(F32) * g_ref[t * 32 : t * 32 + 32, :]
        c_ref[pl.ds(pl.multiple_of(m * 32, 32), 32), :] = total
        return carry

    lax.fori_loop(0, 40, contract, 0)
    xe_buf[0] = c_ref[pl.ds(0, 80, stride=16), :]
    xe_buf[1] = c_ref[pl.ds(15, 80, stride=16), :]

    second = [
        remote(xe_buf.at[0], xe_got.at[1], send2.at[0], recv2.at[1], {"tx": west, "ty": ty, "mem": mem}),
        remote(xe_buf.at[1], xe_got.at[0], send2.at[1], recv2.at[0], {"tx": east, "ty": ty, "mem": mem}),
        remote(ce_buf, ce_got, send2.at[2], recv2.at[2], {"tx": tx, "ty": over, "mem": mem}),
        remote(cc_buf.at[0], cc_got.at[1], send2.at[3], recv2.at[4], {"tx": west, "ty": over, "mem": mem}),
        remote(cc_buf.at[1], cc_got.at[0], send2.at[4], recv2.at[3], {"tx": east, "ty": over, "mem": mem}),
    ]
    for copy in second:
        copy.start()

    row32 = lax.broadcasted_iota(jnp.int32, (32, 128), 0) % 16
    lane32 = lax.broadcasted_iota(jnp.int32, (32, 128), 1)

    def along_x(c):
        up = jnp.where(row32 == 0, 0.0, pltpu.roll(c, 1, 0))
        down = jnp.where(row32 == 15, 0.0, pltpu.roll(c, 31, 0))
        return 0.5 * c + 0.25 * (up + down)

    def along_y(c, lane):
        left = jnp.where(lane == 0, 0.0, pltpu.roll(c, 1, 1))
        right = jnp.where(lane == 127, 0.0, pltpu.roll(c, 127, 1))
        return 0.5 * c + 0.25 * (left + right)

    def inside(m, carry):
        at = pl.ds(pl.multiple_of(m * 32, 32), 32)
        f_ref[at, :] = along_y(along_x(c_ref[at, :]), lane32)
        return carry

    lax.fori_loop(0, 40, inside, 0)

    for copy in second:
        copy.wait_send()
    remote(xe_buf.at[0], xe_got.at[1], send2.at[0], recv2.at[1], {"tx": west, "ty": ty, "mem": mem}).wait_recv()
    remote(xe_buf.at[1], xe_got.at[0], send2.at[1], recv2.at[0], {"tx": east, "ty": ty, "mem": mem}).wait_recv()
    remote(ce_buf, ce_got, send2.at[2], recv2.at[2], {"tx": tx, "ty": over, "mem": mem}).wait_recv()
    remote(cc_buf.at[0], cc_got.at[1], send2.at[3], recv2.at[4], {"tx": west, "ty": over, "mem": mem}).wait_recv()
    remote(cc_buf.at[1], cc_got.at[0], send2.at[4], recv2.at[3], {"tx": east, "ty": over, "mem": mem}).wait_recv()

    lane80 = lax.broadcasted_iota(jnp.int32, (80, 128), 1)
    hx_ref[0] = along_y(xe_got[0], lane80) * (0.25 * has_west)
    hx_ref[1] = along_y(xe_got[1], lane80) * (0.25 * has_east)
    side = along_x(ce_got[...])
    for v in range(2):
        before = cc_got[0, v : v + 1, :] * (0.25 * has_west)
        behind = cc_got[1, v : v + 1, :] * (0.25 * has_east)
        here = lax.broadcasted_iota(jnp.int32, (32, 128), 0)
        side = side + jnp.where(here == v * 16, before, 0.0) + jnp.where(here == v * 16 + 15, behind, 0.0)
    hy_ref[...] = side * 0.25

    def finish(m, carry):
        at = pl.ds(pl.multiple_of(m * 32, 32), 32)
        f = f_ref[at, :] + jnp.where(lane32 == edge, pltpu.roll(hy_ref[...], lax.rem(edge - m + 128, 128), 1), 0.0)
        low, high = [], []
        for v in range(2):
            low.append(jnp.broadcast_to(hx_ref[0, pl.ds(2 * m + v, 1), :], (16, 128)))
            high.append(jnp.broadcast_to(hx_ref[1, pl.ds(2 * m + v, 1), :], (16, 128)))
        f = f + jnp.where(row32 == 0, jnp.concatenate(low, axis=0), 0.0)
        f = f + jnp.where(row32 == 15, jnp.concatenate(high, axis=0), 0.0)
        out_ref[m] = f.astype(BF16)
        return carry

    lax.fori_loop(0, 40, finish, 0)

    for copy in first:
        copy.wait_send()

    group(0, 0, TILES - 1).wait_send()


def body(obs_value, obs_frac, obs_cell, obs_layer, obs_tile, obs_length, ensemble):
    square = (ROWS, 128)
    dma = pltpu.SemaphoreType.DMA
    out = pl.pallas_call(
        all_kernel,
        out_shape=pltpu.VMEM((40, 32, 128), BF16),
        in_specs=[pl.BlockSpec(memory_space=pltpu.SMEM)] + [pl.BlockSpec(memory_space=pl.ANY)] * 6,
        out_specs=VMEM_SPEC,
        scratch_shapes=[
            pltpu.VMEM(square, F32),
            pltpu.VMEM((2, ROWS * 128), F32),
            pltpu.VMEM(square, jnp.int32),
            pltpu.VMEM(square, jnp.int32),
            pltpu.VMEM(square, jnp.int32),
            pltpu.VMEM(square, F32),
            pltpu.VMEM(square, F32),
            pltpu.VMEM((384, 256), F32),
            pltpu.VMEM((TILES, 6, 128), F32),
            pltpu.VMEM((TILES, 6, 128), F32),
            pltpu.VMEM((272, 192), F32),
            pltpu.VMEM((40, 192, 128), BF16),
            pltpu.VMEM((192, 128), F32),
            pltpu.VMEM((192, 128), F32),
            pltpu.VMEM((192, 128), F32),
            pltpu.VMEM((192, 128), F32),
            pltpu.VMEM((12, 128), F32),
            pltpu.VMEM((2, 12, 128), F32),
            pltpu.VMEM((8, 256), F32),
            pltpu.VMEM((2, 8, 256), F32),
            pltpu.VMEM((8, 256), F32),
            pltpu.VMEM((2, 8, 256), F32),
            pltpu.VMEM((192, 128), F32),
            pltpu.VMEM((1280, 128), F32),
            pltpu.VMEM((1280, 128), F32),
            pltpu.VMEM((2, 80, 128), F32),
            pltpu.VMEM((2, 80, 128), F32),
            pltpu.VMEM((32, 128), F32),
            pltpu.VMEM((32, 128), F32),
            pltpu.VMEM((2, 2, 128), F32),
            pltpu.VMEM((2, 2, 128), F32),
            pltpu.VMEM((2, 80, 128), F32),
            pltpu.VMEM((32, 128), F32),
            dma((5,)),
            dma,
            dma,
            dma((8,)),
            dma((7,)),
            dma((7,)),
            dma((5,)),
            dma((5,)),
        ],
        compiler_params=pltpu.CompilerParams(collective_id=0, has_side_effects=True),
    )(
        obs_length,
        obs_value.reshape(square),
        obs_frac,
        obs_cell.reshape(square),
        obs_layer.reshape(square),
        obs_tile.reshape(square),
        ensemble.reshape(40, 192, 128),
    )
    return out.reshape(40, 2, 16, 128)


def solution(mesh):
    placed = (
        P(("tx", "ty", "mem")),
        P(None, ("tx", "ty", "mem")),
        P(("tx", "ty", "mem")),
        P(("tx", "ty", "mem")),
        P(("tx", "ty", "mem")),
        P(("tx", "ty", "mem")),
        P("mem", None, None, "tx", "ty"),
    )
    return jax.shard_map(
        body, mesh=mesh, in_specs=placed, out_specs=P("mem", None, "tx", "ty"), check_vma=False
    )
```

```python
import functools

import jax
import jax.numpy as jnp
from jax import lax
from jax.experimental import pallas as pl
from jax.experimental.pallas import tpu as pltpu
from jax.sharding import PartitionSpec as P

F32 = jnp.float32
BF16 = jnp.bfloat16
MESH_ID = pl.DeviceIdType.MESH
VMEM_SPEC = pl.BlockSpec(memory_space=pltpu.VMEM)
SLOT = 64
TILES = 128
CHUNKS = 3
ROWS = 64
DEAD = 1000.0


def packed_iota(groups, shift):
    a = lax.broadcasted_iota(jnp.int32, (groups, 16, 128), 0)
    b = lax.broadcasted_iota(jnp.int32, (groups, 16, 128), 1)
    return (a * 16 + b + shift).astype(F32).astype(BF16)


def spread_row(row):
    return jnp.broadcast_to(row, (16, 128)).astype(BF16)[None]


def two_parts(x):
    hi = x.astype(BF16).astype(F32)
    return hi, x - hi


def dot_t(a, b):
    return lax.dot_general(a, b, (((1,), (1,)), ((), ())), preferred_element_type=F32)


def dot_n(a, b):
    return lax.dot_general(a, b, (((1,), (0,)), ((), ())), preferred_element_type=F32)


def rank_stage(length, z_own, tile_ref, d_ref, s_ref):
    i = lax.broadcasted_iota(jnp.int32, (128, 256), 0)
    j = lax.broadcasted_iota(jnp.int32, (128, 256), 1)
    before = jnp.where((i < j) | (j >= 128), 1.0, 0.0).astype(BF16)
    tiles_id = lax.broadcasted_iota(jnp.int32, (TILES, 128), 0)
    lane = lax.broadcasted_iota(jnp.int32, (1, 128), 1)
    per = 4

    def step(k, offset):
        for q in range(per):
            r = k * per + q
            t = tile_ref[pl.ds(r, 1), :]
            live = (lane + r * 128) < length
            t = jnp.where(live, t, -1)
            match = tiles_id == t
            both = dot_n(jnp.where(match, 1.0, 0.0).astype(BF16), before)
            rank = jnp.sum(jnp.where(match, both[:, :128] + offset, 0.0), axis=0, keepdims=True)
            offset = offset + both[:, 128:]
            c = jnp.floor(rank * (1.0 / SLOT))
            tf = t.astype(F32)
            t4 = jnp.floor(tf * 0.25)
            z = jnp.floor(t4 * 0.25)
            e = z - z_own.astype(F32) + 6.0
            e = e - 8.0 * jnp.floor(e * 0.125)
            near = jnp.where(e >= 4.0, 1.0, 0.0)
            d = near * 48.0 + c * 16.0 + (e - near * 4.0) * 4.0 + (t4 - z * 4.0)
            d_ref[pl.ds(r, 1), :] = jnp.where(live, d, DEAD)
            s_ref[pl.ds(r, 1), :] = (tf - 4.0 * t4) * SLOT + (rank - c * SLOT)
        return offset

    lax.fori_loop(0, ROWS // per, step, jnp.zeros((TILES, 128), F32))


def pack_stage(near, val_ref, frac_ref, cell_ref, layer_ref, d_ref, s_ref, acc_ref, out_ref):
    d_ids = packed_iota(3, near * 48)
    s_ids = packed_iota(16, 0)
    one = jnp.ones((1, 16, 128), BF16)
    zero = jnp.zeros((1, 16, 128), BF16)
    acc_ref[...] = jnp.zeros_like(acc_ref)
    per = 16

    def step(k, carry):
        rights, highs, lows = [], [], []
        for q in range(per):
            r = k * per + q
            mask = d_ids == spread_row(d_ref[pl.ds(r, 1), :])
            rights.append(jnp.where(s_ids == spread_row(s_ref[pl.ds(r, 1), :]), one, zero).reshape(256, 128))
            v = val_ref[pl.ds(r, 1), :]
            fx = frac_ref[0:1, pl.ds(pl.multiple_of(r * 128, 128), 128)]
            fy = frac_ref[1:2, pl.ds(pl.multiple_of(r * 128, 128), 128)]
            pos = layer_ref[pl.ds(r, 1), :] * 2048 + cell_ref[pl.ds(r, 1), :]
            pos_low = (pos & 255).astype(F32)
            pos_high = pos.astype(F32) - pos_low
            parts = [two_parts(v), (pos_high, pos_low), two_parts(fx), two_parts(fy)]
            for into, p in ((highs, 0), (lows, 1)):
                into.append(
                    jnp.concatenate(
                        [jnp.where(mask, spread_row(w[p]), zero).reshape(48, 128) for w in parts],
                        axis=0,
                    )
                )
        right = jnp.concatenate(rights, axis=1)
        acc_ref[...] += dot_t(jnp.concatenate(highs, axis=1), right) + dot_t(
            jnp.concatenate(lows, axis=1), right
        )
        return carry

    lax.fori_loop(0, ROWS // per, step, 0)
    low = lax.broadcasted_iota(jnp.int32, (16, 128), 1) < SLOT
    for c in range(CHUNKS):
        for col in range(2):
            plain = [acc_ref[w * 48 + c * 16 : w * 48 + c * 16 + 16, col * 128 : col * 128 + 128] for w in range(4)]
            moved = [pltpu.roll(w, SLOT, 1) for w in plain]
            for half in range(2):
                at = (2 * col + half) * 32 + near * 16
                for h in range(2):
                    first, last = (plain[2 * h], moved[2 * h + 1]) if half == 0 else (moved[2 * h], plain[2 * h + 1])
                    out_ref[at : at + 16, 2 * c + h, :] = jnp.where(low, first, last)


def peers(tx, ty):
    z, y, x = tx // 8, (tx // 2) % 4, (tx % 2) * 2 + ty
    z_parts = [((z + dz) % 8) * 8 for dz in range(8)]

    def pair(q):
        px = (x + q) % 4
        py = (y + q // 4) % 4
        return py, px

    return z_parts, pair


def spread_block(r_ref, first, acc_ref):
    lane = lax.broadcasted_iota(jnp.int32, (8, 128), 1)
    low = lane < SLOT
    x_ids = packed_iota(12, 0)
    y_ids = packed_iota(8, 0)
    rim_id = lax.broadcasted_iota(jnp.int32, (16, 128), 0)
    one = jnp.ones((1, 16, 128), BF16)
    zero = jnp.zeros((1, 16, 128), BF16)

    def both(j):
        a = r_ref[pl.ds(first, 8), j, :]
        b = r_ref[pl.ds(first + 8, 8), j, :]
        return jnp.where(low, a, pltpu.roll(b, SLOT, 1)), jnp.where(low, pltpu.roll(a, SLOT, 1), b)

    for c in range(CHUNKS):
        v, pos = both(2 * c)
        fx, fy = both(2 * c + 1)
        key = jnp.floor(pos * (1.0 / 128.0))
        cy = pos - key * 128.0
        v1 = v * fx
        v0 = v * (1.0 - fx)
        gy = 1.0 - fy
        q = [two_parts(u) for u in (v0 * gy, v0 * fy, v1 * gy, v1 * fy)]
        last = cy == 127.0
        rims = [[jnp.where(last, q[1][p], 0.0), jnp.where(last, q[3][p], 0.0)] for p in range(2)]
        rights, lefts = [], [[], []]
        for r in range(8):
            def row(u):
                return u[r : r + 1, :]
            rights.append(jnp.where(x_ids == spread_row(row(key)), one, zero).reshape(192, 128))
            here = spread_row(row(cy))
            m0 = y_ids == here
            m1 = y_ids == spread_row(row(cy) + 1.0)
            for p in range(2):
                pieces = []
                for a in range(2):
                    w0 = spread_row(row(q[2 * a][p]))
                    w1 = spread_row(row(q[2 * a + 1][p]))
                    pieces.append(jnp.where(m0, w0, jnp.where(m1, w1, zero)).reshape(128, 128))
                edge = jnp.where(
                    rim_id == 0,
                    jnp.broadcast_to(row(rims[p][0]), (16, 128)),
                    jnp.where(rim_id == 1, jnp.broadcast_to(row(rims[p][1]), (16, 128)), 0.0),
                ).astype(BF16)
                lefts[p].append(jnp.concatenate(pieces + [edge], axis=0))
        right = jnp.concatenate(rights, axis=1)
        acc_ref[...] += dot_t(jnp.concatenate(lefts[0], axis=1), right) + dot_t(
            jnp.concatenate(lefts[1], axis=1), right
        )


def remote(src, dst, send_sem, recv_sem, where):
    return pltpu.make_async_remote_copy(
        src_ref=src, dst_ref=dst, send_sem=send_sem, recv_sem=recv_sem, device_id=where, device_id_type=MESH_ID
    )


def edge_columns(ens_ref, edge, out_ref):
    k = lax.broadcasted_iota(jnp.int32, (1024, 128), 0)
    col = lax.broadcasted_iota(jnp.int32, (1024, 128), 1)
    total = jnp.zeros((192, 128), F32)
    for g in range(5):
        left = jnp.concatenate([ens_ref[8 * g + m] for m in range(8)], axis=1)
        pick = ((k % 128 == edge) & (k // 128 + 8 * g == col)).astype(F32).astype(BF16)
        total = total + dot_n(left, pick)
    out_ref[...] = total


def edge_rows(ens_ref, out_ref):
    def step(m, carry):
        for k in range(12):
            block = ens_ref[m, k * 16 : k * 16 + 16, :].astype(F32)
            out_ref[0, k, pl.ds(m, 1), :] = block[0:1, :]
            out_ref[1, k, pl.ds(m, 1), :] = block[15:16, :]
        return carry

    lax.fori_loop(0, 40, step, 0)


def all_kernel(
    length_ref, val_hbm, frac_hbm, cell_hbm, layer_hbm, tile_hbm, ens_hbm, out_ref,
    val_ref, frac_ref, cell_ref, layer_ref, tile_ref,
    d_ref, s_ref, acc_ref, sbuf, rbuf, grid_ref, ens_ref, col_ref, rows_ref,
    part_buf, part_got, next_buf, east_buf, east_got, north_buf, north_got, corner_buf, corner_got,
    g_ref, c_ref, f_ref, xe_buf, xe_got, ce_buf, ce_got, cc_buf, cc_got, hx_ref, hy_ref,
    in_sem, ens_sem, send_sem, recv_sem, send1, recv1, send2, recv2,
):
    tx = lax.axis_index("tx")
    ty = lax.axis_index("ty")
    mem = lax.axis_index("mem")
    n_tx = lax.axis_size("tx")
    east = lax.rem(tx + 1, n_tx)
    west = lax.rem(tx + n_tx - 1, n_tx)
    over = 1 - ty
    twin = 1 - mem
    barrier = pltpu.get_barrier_semaphore()

    z_parts, pair = peers(tx, ty)

    def over_peers(act, near):
        steps = (0, 1, 7, 6) if near else (4, 3, 5, 2)

        def some(q, first):
            py, px = pair(q)
            for n in range(first, 4):
                dz = steps[n]
                place = px * 32 + (dz + 6) % 8 * 4 + py
                act(near * 64 + q * 4 + n, z_parts[dz] + py * 2 + px // 2, px % 2, place)

        some(0, near)

        def step(q, carry):
            some(q, 0)
            return carry

        lax.fori_loop(1, 16, step, 0)

    def copy_in(src, dst, i):
        copy = pltpu.make_async_copy(src, dst, in_sem.at[i])
        copy.start()
        return copy

    tile_in = copy_in(tile_hbm, tile_ref, 0)
    others_in = [
        copy_in(val_hbm, val_ref, 1),
        copy_in(frac_hbm, frac_ref, 2),
        copy_in(cell_hbm, cell_ref, 3),
        copy_in(layer_hbm, layer_ref, 4),
    ]
    ens_copy = pltpu.make_async_copy(ens_hbm, ens_ref, ens_sem)
    ens_copy.start()

    def greet(i, px, py, at):
        pl.semaphore_signal(barrier, inc=1, device_id={"tx": px, "ty": py, "mem": mem}, device_id_type=MESH_ID)

    over_peers(greet, 0)
    over_peers(greet, 1)
    for px, py in ((tx, ty), (west, ty), (tx, over), (west, over)):
        pl.semaphore_signal(barrier, inc=1, device_id={"tx": px, "ty": py, "mem": twin}, device_id_type=MESH_ID)
    tile_in.wait()
    rank_stage(length_ref[0], tx // 8, tile_ref, d_ref, s_ref)
    for copy in others_in:
        copy.wait()
    packing = (val_ref, frac_ref, cell_ref, layer_ref, d_ref, s_ref, acc_ref, sbuf)
    pack_stage(0, *packing)

    pl.semaphore_wait(barrier, TILES - 1 + 4)

    def message(i, px, py, at):
        return remote(sbuf.at[at], rbuf.at[i], send_sem, recv_sem.at[i // 16], {"tx": px, "ty": py, "mem": mem})

    def group(k, first, count):
        at = pl.ds(first, count)
        return remote(sbuf.at[at], rbuf.at[at], send_sem, recv_sem.at[k], {"tx": west, "ty": ty, "mem": mem})

    over_peers(lambda *peer: message(*peer).start(), 0)
    pack_stage(1, *packing)
    over_peers(lambda *peer: message(*peer).start(), 1)
    py, px = pair(0)
    rbuf[pl.ds(64, 1)] = sbuf[pl.ds(px * 32 + 24 + py, 1)]
    edge = (1 - ty) * 127
    ens_copy.wait()
    edge_columns(ens_ref, edge, col_ref)
    edge_rows(ens_ref, rows_ref)

    grid_ref[...] = jnp.zeros_like(grid_ref)

    def gather(k, carry):
        group(k, k * 16, 16).wait_recv()
        spread_block(rbuf, k * 16, grid_ref)
        return carry

    lax.fori_loop(0, 4, gather, 0)
    group(4, 65, 15).wait_recv()
    spread_block(rbuf, 64, grid_ref)
    lax.fori_loop(5, 8, gather, 0)

    row = lax.broadcasted_iota(jnp.int32, (192, 128), 0)
    x_first = (row % 16) == 0
    lane192 = lax.broadcasted_iota(jnp.int32, (192, 128), 1)
    lane256 = lax.broadcasted_iota(jnp.int32, (8, 256), 1)
    row8 = lax.broadcasted_iota(jnp.int32, (8, 256), 0)
    after = grid_ref[128:256, :].T
    mine = grid_ref[0:128, :].T + jnp.where(x_first, 0.0, pltpu.roll(after, 1, 0))
    part_buf[...] = mine
    next_buf[...] = after
    east_buf[...] = next_buf[pl.ds(15, 12, stride=16), :]
    pad = jnp.zeros((8, 64), F32)
    rim0 = jnp.concatenate([jnp.broadcast_to(grid_ref[256:257, :], (8, 192)), pad], axis=1)
    rim1 = jnp.concatenate([jnp.broadcast_to(grid_ref[257:258, :], (8, 192)), pad], axis=1)
    top = row8 == 0
    first256 = (lane256 % 16) == 0
    north_buf[...] = jnp.where(top, rim0 + jnp.where(first256, 0.0, pltpu.roll(rim1, 1, 1)), 0.0)
    corner_buf[...] = jnp.where(top & first256, pltpu.roll(rim1, 241, 1), 0.0)

    first = [remote(part_buf, part_got, send1.at[0], recv1.at[0], {"tx": tx, "ty": ty, "mem": twin})]
    for j in range(2):
        first.append(remote(east_buf, east_got.at[mem], send1.at[1 + j], recv1.at[1 + mem], {"tx": east, "ty": ty, "mem": j}))
        first.append(remote(north_buf, north_got.at[mem], send1.at[3 + j], recv1.at[3 + mem], {"tx": tx, "ty": over, "mem": j}))
        first.append(remote(corner_buf, corner_got.at[mem], send1.at[5 + j], recv1.at[5 + mem], {"tx": east, "ty": over, "mem": j}))
    for copy in first:
        copy.start()
    remote(part_buf, part_got, send1.at[0], recv1.at[0], {"tx": tx, "ty": ty, "mem": twin}).wait_recv()
    for j in range(2):
        remote(east_buf, east_got.at[j], send1.at[1 + j], recv1.at[1 + j], {"tx": east, "ty": ty, "mem": j}).wait_recv()
        remote(north_buf, north_got.at[j], send1.at[3 + j], recv1.at[3 + j], {"tx": tx, "ty": over, "mem": j}).wait_recv()
        remote(corner_buf, corner_got.at[j], send1.at[5 + j], recv1.at[5 + j], {"tx": east, "ty": over, "mem": j}).wait_recv()
    has_west = jnp.where(tx > 0, 1.0, 0.0)
    has_east = jnp.where(tx < n_tx - 1, 1.0, 0.0)
    has_south = jnp.where(ty > 0, 1.0, 0.0)
    rims = (north_got[0] + north_got[1] + (corner_got[0] + corner_got[1]) * has_west) * has_south
    rims = jnp.concatenate([rims, jnp.zeros((120, 256), F32)], axis=0).T
    wall = (east_got[0] + east_got[1]) * has_west
    wall = jnp.broadcast_to(wall[:, None, :], (12, 16, 128)).reshape(192, 128)
    g = part_buf[...] + part_got[...] + rims[0:192, :] + jnp.where(x_first, wall, 0.0)
    g_ref[...] = g
    for n in range(2):
        for v in range(2):
            total = jnp.zeros((40, 128), F32)
            for t in range(6):
                at = (t * 2 + v) * 16 + 15 * n
                total = total + rows_ref[n, t * 2 + v] * g[at : at + 1, :]
            xe_buf[n, v * 40 : v * 40 + 40, :] = total
    second = [
        remote(xe_buf.at[0], xe_got.at[1], send2.at[0], recv2.at[1], {"tx": west, "ty": ty, "mem": mem}),
        remote(xe_buf.at[1], xe_got.at[0], send2.at[1], recv2.at[0], {"tx": east, "ty": ty, "mem": mem}),
        remote(ce_buf, ce_got, send2.at[2], recv2.at[2], {"tx": tx, "ty": over, "mem": mem}),
        remote(cc_buf.at[0], cc_got.at[1], send2.at[3], recv2.at[4], {"tx": west, "ty": over, "mem": mem}),
        remote(cc_buf.at[1], cc_got.at[0], send2.at[4], recv2.at[3], {"tx": east, "ty": over, "mem": mem}),
    ]
    second[0].start()
    second[1].start()
    gcol = jnp.sum(jnp.where(lane192 == edge, g, 0.0), axis=1, keepdims=True)
    ce = jnp.zeros((32, 128), F32)
    for t in range(6):
        ce = ce + col_ref[t * 32 : t * 32 + 32, :] * gcol[t * 32 : t * 32 + 32, :]
    ce_buf[...] = ce
    for v in range(2):
        cc_buf[0, v : v + 1, :] = ce[v * 16 : v * 16 + 1, :]
        cc_buf[1, v : v + 1, :] = ce[v * 16 + 15 : v * 16 + 16, :]

    for copy in second[2:]:
        copy.start()

    def contract(m, carry):
        total = jnp.zeros((32, 128), F32)
        for t in range(6):
            total = total + ens_ref[m, t * 32 : t * 32 + 32, :].astype(F32) * g_ref[t * 32 : t * 32 + 32, :]
        c_ref[pl.ds(pl.multiple_of(m * 32, 32), 32), :] = total
        return carry

    lax.fori_loop(0, 40, contract, 0)
    row32 = lax.broadcasted_iota(jnp.int32, (32, 128), 0) % 16
    lane32 = lax.broadcasted_iota(jnp.int32, (32, 128), 1)

    def along_x(c):
        up = jnp.where(row32 == 0, 0.0, pltpu.roll(c, 1, 0))
        down = jnp.where(row32 == 15, 0.0, pltpu.roll(c, 31, 0))
        return 0.5 * c + 0.25 * (up + down)

    def along_y(c, lane):
        left = jnp.where(lane == 0, 0.0, pltpu.roll(c, 1, 1))
        right = jnp.where(lane == 127, 0.0, pltpu.roll(c, 127, 1))
        return 0.5 * c + 0.25 * (left + right)

    def inside(m, carry):
        at = pl.ds(pl.multiple_of(m * 32, 32), 32)
        f_ref[at, :] = along_y(along_x(c_ref[at, :]), lane32)
        return carry

    lax.fori_loop(0, 40, inside, 0)

    for copy in second:
        copy.wait_send()
    remote(xe_buf.at[0], xe_got.at[1], send2.at[0], recv2.at[1], {"tx": west, "ty": ty, "mem": mem}).wait_recv()
    remote(xe_buf.at[1], xe_got.at[0], send2.at[1], recv2.at[0], {"tx": east, "ty": ty, "mem": mem}).wait_recv()
    remote(ce_buf, ce_got, send2.at[2], recv2.at[2], {"tx": tx, "ty": over, "mem": mem}).wait_recv()
    remote(cc_buf.at[0], cc_got.at[1], send2.at[3], recv2.at[4], {"tx": west, "ty": over, "mem": mem}).wait_recv()
    remote(cc_buf.at[1], cc_got.at[0], send2.at[4], recv2.at[3], {"tx": east, "ty": over, "mem": mem}).wait_recv()

    lane80 = lax.broadcasted_iota(jnp.int32, (80, 128), 1)
    hx_ref[0] = along_y(xe_got[0], lane80) * (0.25 * has_west)
    hx_ref[1] = along_y(xe_got[1], lane80) * (0.25 * has_east)
    side = along_x(ce_got[...])
    for v in range(2):
        before = cc_got[0, v : v + 1, :] * (0.25 * has_west)
        behind = cc_got[1, v : v + 1, :] * (0.25 * has_east)
        here = lax.broadcasted_iota(jnp.int32, (32, 128), 0)
        side = side + jnp.where(here == v * 16, before, 0.0) + jnp.where(here == v * 16 + 15, behind, 0.0)
    hy_ref[...] = side * 0.25

    def finish(m, carry):
        at = pl.ds(pl.multiple_of(m * 32, 32), 32)
        f = f_ref[at, :] + jnp.where(lane32 == edge, pltpu.roll(hy_ref[...], lax.rem(edge - m + 128, 128), 1), 0.0)
        low, high = [], []
        for v in range(2):
            low.append(jnp.broadcast_to(hx_ref[0, pl.ds(v * 40 + m, 1), :], (16, 128)))
            high.append(jnp.broadcast_to(hx_ref[1, pl.ds(v * 40 + m, 1), :], (16, 128)))
        f = f + jnp.where(row32 == 0, jnp.concatenate(low, axis=0), 0.0)
        f = f + jnp.where(row32 == 15, jnp.concatenate(high, axis=0), 0.0)
        out_ref[m] = f.astype(BF16)
        return carry

    lax.fori_loop(0, 40, finish, 0)

    for copy in first:
        copy.wait_send()

    group(0, 0, TILES - 1).wait_send()


def body(obs_value, obs_frac, obs_cell, obs_layer, obs_tile, obs_length, ensemble):
    square = (ROWS, 128)
    dma = pltpu.SemaphoreType.DMA
    out = pl.pallas_call(
        all_kernel,
        out_shape=pltpu.VMEM((40, 32, 128), BF16),
        in_specs=[pl.BlockSpec(memory_space=pltpu.SMEM)] + [pl.BlockSpec(memory_space=pl.ANY)] * 6,
        out_specs=VMEM_SPEC,
        scratch_shapes=[
            pltpu.VMEM(square, F32),
            pltpu.VMEM((2, ROWS * 128), F32),
            pltpu.VMEM(square, jnp.int32),
            pltpu.VMEM(square, jnp.int32),
            pltpu.VMEM(square, jnp.int32),
            pltpu.VMEM(square, F32),
            pltpu.VMEM(square, F32),
            pltpu.VMEM((192, 256), F32),
            pltpu.VMEM((TILES, 6, 128), F32),
            pltpu.VMEM((TILES, 6, 128), F32),
            pltpu.VMEM((272, 192), F32),
            pltpu.VMEM((40, 192, 128), BF16),
            pltpu.VMEM((192, 128), F32),
            pltpu.VMEM((2, 12, 40, 128), F32),
            pltpu.VMEM((192, 128), F32),
            pltpu.VMEM((192, 128), F32),
            pltpu.VMEM((192, 128), F32),
            pltpu.VMEM((12, 128), F32),
            pltpu.VMEM((2, 12, 128), F32),
            pltpu.VMEM((8, 256), F32),
            pltpu.VMEM((2, 8, 256), F32),
            pltpu.VMEM((8, 256), F32),
            pltpu.VMEM((2, 8, 256), F32),
            pltpu.VMEM((192, 128), F32),
            pltpu.VMEM((1280, 128), F32),
            pltpu.VMEM((1280, 128), F32),
            pltpu.VMEM((2, 80, 128), F32),
            pltpu.VMEM((2, 80, 128), F32),
            pltpu.VMEM((32, 128), F32),
            pltpu.VMEM((32, 128), F32),
            pltpu.VMEM((2, 2, 128), F32),
            pltpu.VMEM((2, 2, 128), F32),
            pltpu.VMEM((2, 80, 128), F32),
            pltpu.VMEM((32, 128), F32),
            dma((5,)),
            dma,
            dma,
            dma((8,)),
            dma((7,)),
            dma((7,)),
            dma((5,)),
            dma((5,)),
        ],
        compiler_params=pltpu.CompilerParams(collective_id=0, has_side_effects=True),
    )(
        obs_length,
        obs_value.reshape(square),
        obs_frac,
        obs_cell.reshape(square),
        obs_layer.reshape(square),
        obs_tile.reshape(square),
        ensemble.reshape(40, 192, 128),
    )
    return out.reshape(40, 2, 16, 128)


def solution(mesh):
    placed = (
        P(("tx", "ty", "mem")),
        P(None, ("tx", "ty", "mem")),
        P(("tx", "ty", "mem")),
        P(("tx", "ty", "mem")),
        P(("tx", "ty", "mem")),
        P(("tx", "ty", "mem")),
        P("mem", None, None, "tx", "ty"),
    )
    return jax.shard_map(
        body, mesh=mesh, in_specs=placed, out_specs=P("mem", None, "tx", "ty"), check_vma=False
    )
```

```python
import functools

import jax
import jax.numpy as jnp
from jax import lax
from jax.experimental import pallas as pl
from jax.experimental.pallas import tpu as pltpu
from jax.sharding import PartitionSpec as P

F32 = jnp.float32
BF16 = jnp.bfloat16
MESH_ID = pl.DeviceIdType.MESH
VMEM_SPEC = pl.BlockSpec(memory_space=pltpu.VMEM)
SLOT = 64
TILES = 128
CHUNKS = 3
ROWS = 64
DEAD = 1000.0


def packed_iota(groups, shift):
    a = lax.broadcasted_iota(jnp.int32, (groups, 16, 128), 0)
    b = lax.broadcasted_iota(jnp.int32, (groups, 16, 128), 1)
    return (a * 16 + b + shift).astype(F32).astype(BF16)


def spread_row(row):
    return jnp.broadcast_to(row, (16, 128)).astype(BF16)[None]


def two_parts(x):
    hi = x.astype(BF16).astype(F32)
    return hi, x - hi


def dot_t(a, b):
    return lax.dot_general(a, b, (((1,), (1,)), ((), ())), preferred_element_type=F32)


def dot_n(a, b):
    return lax.dot_general(a, b, (((1,), (0,)), ((), ())), preferred_element_type=F32)


def rank_stage(length, z_own, tile_ref, d_ref, s_ref):
    i = lax.broadcasted_iota(jnp.int32, (128, 256), 0)
    j = lax.broadcasted_iota(jnp.int32, (128, 256), 1)
    before = jnp.where((i < j) | (j >= 128), 1.0, 0.0).astype(BF16)
    tiles_id = lax.broadcasted_iota(jnp.int32, (TILES, 128), 0)
    lane = lax.broadcasted_iota(jnp.int32, (1, 128), 1)
    per = 4

    def step(k, offset):
        for q in range(per):
            r = k * per + q
            t = tile_ref[pl.ds(r, 1), :]
            live = (lane + r * 128) < length
            t = jnp.where(live, t, -1)
            match = tiles_id == t
            both = dot_n(jnp.where(match, 1.0, 0.0).astype(BF16), before)
            rank = jnp.sum(jnp.where(match, both[:, :128] + offset, 0.0), axis=0, keepdims=True)
            offset = offset + both[:, 128:]
            c = jnp.floor(rank * (1.0 / SLOT))
            tf = t.astype(F32)
            t4 = jnp.floor(tf * 0.25)
            z = jnp.floor(t4 * 0.25)
            e = z - z_own.astype(F32) + 6.0
            e = e - 8.0 * jnp.floor(e * 0.125)
            near = jnp.where(e >= 4.0, 1.0, 0.0)
            d = near * 48.0 + c * 16.0 + (e - near * 4.0) * 4.0 + (t4 - z * 4.0)
            d_ref[pl.ds(r, 1), :] = jnp.where(live, d, DEAD)
            s_ref[pl.ds(r, 1), :] = (tf - 4.0 * t4) * SLOT + (rank - c * SLOT)
        return offset

    lax.fori_loop(0, ROWS // per, step, jnp.zeros((TILES, 128), F32))


def pack_stage(near, val_ref, frac_ref, cell_ref, layer_ref, d_ref, s_ref, acc_ref, out_ref):
    d_ids = packed_iota(3, near * 48)
    s_ids = packed_iota(16, 0)
    one = jnp.ones((1, 16, 128), BF16)
    zero = jnp.zeros((1, 16, 128), BF16)
    acc_ref[...] = jnp.zeros_like(acc_ref)
    per = 16

    def step(k, carry):
        rights, highs, lows = [], [], []
        for q in range(per):
            r = k * per + q
            mask = d_ids == spread_row(d_ref[pl.ds(r, 1), :])
            rights.append(jnp.where(s_ids == spread_row(s_ref[pl.ds(r, 1), :]), one, zero).reshape(256, 128))
            v = val_ref[pl.ds(r, 1), :]
            fx = frac_ref[0:1, pl.ds(pl.multiple_of(r * 128, 128), 128)]
            fy = frac_ref[1:2, pl.ds(pl.multiple_of(r * 128, 128), 128)]
            pos = layer_ref[pl.ds(r, 1), :] * 2048 + cell_ref[pl.ds(r, 1), :]
            pos_low = (pos & 255).astype(F32)
            pos_high = pos.astype(F32) - pos_low
            parts = [two_parts(v), (pos_high, pos_low), two_parts(fx), two_parts(fy)]
            for into, p in ((highs, 0), (lows, 1)):
                into.append(
                    jnp.concatenate(
                        [jnp.where(mask, spread_row(w[p]), zero).reshape(48, 128) for w in parts],
                        axis=0,
                    )
                )
        total = jnp.zeros((384, 256), F32)
        for part in (slice(0, per // 2), slice(per // 2, per)):
            left = jnp.concatenate(
                [jnp.concatenate(highs[part], axis=1), jnp.concatenate(lows[part], axis=1)], axis=0
            )
            total = total + dot_t(left, jnp.concatenate(rights[part], axis=1))
        acc_ref[...] += total[:192] + total[192:]
        return carry

    lax.fori_loop(0, ROWS // per, step, 0)
    low = lax.broadcasted_iota(jnp.int32, (16, 128), 1) < SLOT
    for c in range(CHUNKS):
        for col in range(2):
            plain = [acc_ref[w * 48 + c * 16 : w * 48 + c * 16 + 16, col * 128 : col * 128 + 128] for w in range(4)]
            moved = [pltpu.roll(w, SLOT, 1) for w in plain]
            for half in range(2):
                at = (2 * col + half) * 32 + near * 16
                for h in range(2):
                    first, last = (plain[2 * h], moved[2 * h + 1]) if half == 0 else (moved[2 * h], plain[2 * h + 1])
                    out_ref[at : at + 16, 2 * c + h, :] = jnp.where(low, first, last)


def peers(tx, ty):
    z, y, x = tx // 8, (tx // 2) % 4, (tx % 2) * 2 + ty
    z_parts = [((z + dz) % 8) * 8 for dz in range(8)]

    def pair(q):
        px = (x + q) % 4
        py = (y + q // 4) % 4
        return py, px

    return z_parts, pair


def spread_block(r_ref, first, acc_ref):
    lane = lax.broadcasted_iota(jnp.int32, (8, 128), 1)
    low = lane < SLOT
    x_ids = packed_iota(12, 0)
    y_ids = packed_iota(8, 0)
    rim_id = lax.broadcasted_iota(jnp.int32, (16, 128), 0)
    one = jnp.ones((1, 16, 128), BF16)
    zero = jnp.zeros((1, 16, 128), BF16)

    def both(j):
        a = r_ref[pl.ds(first, 8), j, :]
        b = r_ref[pl.ds(first + 8, 8), j, :]
        return jnp.where(low, a, pltpu.roll(b, SLOT, 1)), jnp.where(low, pltpu.roll(a, SLOT, 1), b)

    for c in range(CHUNKS):
        v, pos = both(2 * c)
        fx, fy = both(2 * c + 1)
        key = jnp.floor(pos * (1.0 / 128.0))
        cy = pos - key * 128.0
        v1 = v * fx
        v0 = v * (1.0 - fx)
        gy = 1.0 - fy
        q = [two_parts(u) for u in (v0 * gy, v0 * fy, v1 * gy, v1 * fy)]
        last = cy == 127.0
        rims = [[jnp.where(last, q[1][p], 0.0), jnp.where(last, q[3][p], 0.0)] for p in range(2)]
        rights, lefts = [], [[], []]
        for r in range(8):
            def row(u):
                return u[r : r + 1, :]
            rights.append(jnp.where(x_ids == spread_row(row(key)), one, zero).reshape(192, 128))
            here = spread_row(row(cy))
            m0 = y_ids == here
            m1 = y_ids == spread_row(row(cy) + 1.0)
            for p in range(2):
                pieces = []
                for a in range(2):
                    w0 = spread_row(row(q[2 * a][p]))
                    w1 = spread_row(row(q[2 * a + 1][p]))
                    pieces.append(jnp.where(m0, w0, jnp.where(m1, w1, zero)).reshape(128, 128))
                edge = jnp.where(
                    rim_id == 0,
                    jnp.broadcast_to(row(rims[p][0]), (16, 128)),
                    jnp.where(rim_id == 1, jnp.broadcast_to(row(rims[p][1]), (16, 128)), 0.0),
                ).astype(BF16)
                lefts[p].append(jnp.concatenate(pieces + [edge], axis=0))
        right = jnp.concatenate(rights, axis=1)
        acc_ref[...] += dot_t(jnp.concatenate(lefts[0], axis=1), right) + dot_t(
            jnp.concatenate(lefts[1], axis=1), right
        )


def remote(src, dst, send_sem, recv_sem, where):
    return pltpu.make_async_remote_copy(
        src_ref=src, dst_ref=dst, send_sem=send_sem, recv_sem=recv_sem, device_id=where, device_id_type=MESH_ID
    )


def edge_columns(ens_ref, edge, out_ref):
    k = lax.broadcasted_iota(jnp.int32, (1024, 128), 0)
    col = lax.broadcasted_iota(jnp.int32, (1024, 128), 1)
    total = jnp.zeros((192, 128), F32)
    for g in range(5):
        left = jnp.concatenate([ens_ref[8 * g + m] for m in range(8)], axis=1)
        pick = ((k % 128 == edge) & (k // 128 + 8 * g == col)).astype(F32).astype(BF16)
        total = total + dot_n(left, pick)
    out_ref[...] = total


def edge_rows(ens_ref, out_ref):
    def step(m, carry):
        for k in range(12):
            block = ens_ref[m, k * 16 : k * 16 + 16, :].astype(F32)
            out_ref[0, k, pl.ds(m, 1), :] = block[0:1, :]
            out_ref[1, k, pl.ds(m, 1), :] = block[15:16, :]
        return carry

    lax.fori_loop(0, 40, step, 0)


def all_kernel(
    length_ref, val_hbm, frac_hbm, cell_hbm, layer_hbm, tile_hbm, ens_hbm, out_ref,
    val_ref, frac_ref, cell_ref, layer_ref, tile_ref,
    d_ref, s_ref, acc_ref, sbuf, rbuf, grid_ref, ens_ref, col_ref, rows_ref,
    part_buf, part_got, next_buf, east_buf, east_got, north_buf, north_got, corner_buf, corner_got,
    g_ref, c_ref, f_ref, xe_buf, xe_got, ce_buf, ce_got, cc_buf, cc_got, hx_ref, hy_ref,
    in_sem, ens_sem, send_sem, recv_sem, send1, recv1, send2, recv2,
):
    tx = lax.axis_index("tx")
    ty = lax.axis_index("ty")
    mem = lax.axis_index("mem")
    n_tx = lax.axis_size("tx")
    east = lax.rem(tx + 1, n_tx)
    west = lax.rem(tx + n_tx - 1, n_tx)
    over = 1 - ty
    twin = 1 - mem
    barrier = pltpu.get_barrier_semaphore()

    z_parts, pair = peers(tx, ty)

    def over_peers(act, near):
        steps = (1, 7, 6, 0) if near else (4, 3, 5, 2)

        def some(q, count):
            py, px = pair(q)
            for n in range(count):
                dz = steps[n]
                place = px * 32 + (dz + 6) % 8 * 4 + py
                act(near * 4 + (15 - q) // 4, (15 - q) % 4 * 4 + n, z_parts[dz] + py * 2 + px // 2, px % 2, place)

        def step(i, carry):
            some(15 - i, 4)
            return carry

        lax.fori_loop(0, 15, step, 0)
        some(0, 4 - near)

    def copy_in(src, dst, i):
        copy = pltpu.make_async_copy(src, dst, in_sem.at[i])
        copy.start()
        return copy

    tile_in = copy_in(tile_hbm, tile_ref, 0)
    others_in = [
        copy_in(val_hbm, val_ref, 1),
        copy_in(frac_hbm, frac_ref, 2),
        copy_in(cell_hbm, cell_ref, 3),
        copy_in(layer_hbm, layer_ref, 4),
    ]
    ens_copy = pltpu.make_async_copy(ens_hbm, ens_ref, ens_sem)
    ens_copy.start()

    def greet(k, n, px, py, at):
        pl.semaphore_signal(barrier, inc=1, device_id={"tx": px, "ty": py, "mem": mem}, device_id_type=MESH_ID)

    over_peers(greet, 0)
    over_peers(greet, 1)
    for px, py in ((tx, ty), (west, ty), (tx, over), (west, over)):
        pl.semaphore_signal(barrier, inc=1, device_id={"tx": px, "ty": py, "mem": twin}, device_id_type=MESH_ID)
    tile_in.wait()
    rank_stage(length_ref[0], tx // 8, tile_ref, d_ref, s_ref)
    for copy in others_in:
        copy.wait()
    packing = (val_ref, frac_ref, cell_ref, layer_ref, d_ref, s_ref, acc_ref, sbuf)
    pack_stage(0, *packing)

    pl.semaphore_wait(barrier, TILES - 1 + 4)

    def message(k, n, px, py, at):
        there = {"tx": px, "ty": py, "mem": mem}
        return remote(sbuf.at[at], rbuf.at[k * 16 + n], send_sem, recv_sem.at[k * 2 + n // 15], there)

    def group(sem, first, count):
        at = pl.ds(first, count)
        return remote(sbuf.at[at], rbuf.at[at], send_sem, sem, {"tx": west, "ty": ty, "mem": mem})

    over_peers(lambda *peer: message(*peer).start(), 0)
    pack_stage(1, *packing)
    over_peers(lambda *peer: message(*peer).start(), 1)
    py, px = pair(0)
    rbuf[pl.ds(127, 1)] = sbuf[pl.ds(px * 32 + 24 + py, 1)]
    edge = (1 - ty) * 127
    ens_copy.wait()
    edge_columns(ens_ref, edge, col_ref)
    edge_rows(ens_ref, rows_ref)

    grid_ref[...] = jnp.zeros_like(grid_ref)

    def gather(k, carry):
        group(recv_sem.at[k * 2], k * 16, 15).wait_recv()

        @pl.when(k < 7)
        def _():
            group(recv_sem.at[k * 2 + 1], k * 16 + 15, 1).wait_recv()

        spread_block(rbuf, k * 16, grid_ref)
        return carry

    lax.fori_loop(0, 8, gather, 0)

    row = lax.broadcasted_iota(jnp.int32, (192, 128), 0)
    x_first = (row % 16) == 0
    lane192 = lax.broadcasted_iota(jnp.int32, (192, 128), 1)
    lane256 = lax.broadcasted_iota(jnp.int32, (8, 256), 1)
    row8 = lax.broadcasted_iota(jnp.int32, (8, 256), 0)
    after = grid_ref[128:256, :].T
    mine = grid_ref[0:128, :].T + jnp.where(x_first, 0.0, pltpu.roll(after, 1, 0))
    part_buf[...] = mine
    next_buf[...] = after
    east_buf[...] = next_buf[pl.ds(15, 12, stride=16), :]
    pad = jnp.zeros((8, 64), F32)
    rim0 = jnp.concatenate([jnp.broadcast_to(grid_ref[256:257, :], (8, 192)), pad], axis=1)
    rim1 = jnp.concatenate([jnp.broadcast_to(grid_ref[257:258, :], (8, 192)), pad], axis=1)
    top = row8 == 0
    first256 = (lane256 % 16) == 0
    north_buf[...] = jnp.where(top, rim0 + jnp.where(first256, 0.0, pltpu.roll(rim1, 1, 1)), 0.0)
    corner_buf[...] = jnp.where(top & first256, pltpu.roll(rim1, 241, 1), 0.0)

    first = [remote(part_buf, part_got, send1.at[0], recv1.at[0], {"tx": tx, "ty": ty, "mem": twin})]
    for j in range(2):
        first.append(remote(east_buf, east_got.at[mem], send1.at[1 + j], recv1.at[1 + mem], {"tx": east, "ty": ty, "mem": j}))
        first.append(remote(north_buf, north_got.at[mem], send1.at[3 + j], recv1.at[3 + mem], {"tx": tx, "ty": over, "mem": j}))
        first.append(remote(corner_buf, corner_got.at[mem], send1.at[5 + j], recv1.at[5 + mem], {"tx": east, "ty": over, "mem": j}))
    for copy in first:
        copy.start()
    remote(part_buf, part_got, send1.at[0], recv1.at[0], {"tx": tx, "ty": ty, "mem": twin}).wait_recv()
    for j in range(2):
        remote(east_buf, east_got.at[j], send1.at[1 + j], recv1.at[1 + j], {"tx": east, "ty": ty, "mem": j}).wait_recv()
        remote(north_buf, north_got.at[j], send1.at[3 + j], recv1.at[3 + j], {"tx": tx, "ty": over, "mem": j}).wait_recv()
        remote(corner_buf, corner_got.at[j], send1.at[5 + j], recv1.at[5 + j], {"tx": east, "ty": over, "mem": j}).wait_recv()
    has_west = jnp.where(tx > 0, 1.0, 0.0)
    has_east = jnp.where(tx < n_tx - 1, 1.0, 0.0)
    has_south = jnp.where(ty > 0, 1.0, 0.0)
    rims = (north_got[0] + north_got[1] + (corner_got[0] + corner_got[1]) * has_west) * has_south
    rims = jnp.concatenate([rims, jnp.zeros((120, 256), F32)], axis=0).T
    wall = (east_got[0] + east_got[1]) * has_west
    wall = jnp.broadcast_to(wall[:, None, :], (12, 16, 128)).reshape(192, 128)
    g = part_buf[...] + part_got[...] + rims[0:192, :] + jnp.where(x_first, wall, 0.0)
    g_ref[...] = g
    for n in range(2):
        for v in range(2):
            total = jnp.zeros((40, 128), F32)
            for t in range(6):
                at = (t * 2 + v) * 16 + 15 * n
                total = total + rows_ref[n, t * 2 + v] * g[at : at + 1, :]
            xe_buf[n, v * 40 : v * 40 + 40, :] = total
    second = [
        remote(xe_buf.at[0], xe_got.at[1], send2.at[0], recv2.at[1], {"tx": west, "ty": ty, "mem": mem}),
        remote(xe_buf.at[1], xe_got.at[0], send2.at[1], recv2.at[0], {"tx": east, "ty": ty, "mem": mem}),
        remote(ce_buf, ce_got, send2.at[2], recv2.at[2], {"tx": tx, "ty": over, "mem": mem}),
        remote(cc_buf.at[0], cc_got.at[1], send2.at[3], recv2.at[4], {"tx": west, "ty": over, "mem": mem}),
        remote(cc_buf.at[1], cc_got.at[0], send2.at[4], recv2.at[3], {"tx": east, "ty": over, "mem": mem}),
    ]
    second[0].start()
    second[1].start()
    gcol = jnp.sum(jnp.where(lane192 == edge, g, 0.0), axis=1, keepdims=True)
    ce = jnp.zeros((32, 128), F32)
    for t in range(6):
        ce = ce + col_ref[t * 32 : t * 32 + 32, :] * gcol[t * 32 : t * 32 + 32, :]
    ce_buf[...] = ce
    for v in range(2):
        cc_buf[0, v : v + 1, :] = ce[v * 16 : v * 16 + 1, :]
        cc_buf[1, v : v + 1, :] = ce[v * 16 + 15 : v * 16 + 16, :]

    for copy in second[2:]:
        copy.start()

    def contract(b, carry):
        for m in range(4):
            total = jnp.zeros((32, 128), F32)
            for t in range(6):
                total = total + ens_ref[b * 4 + m, t * 32 : t * 32 + 32, :].astype(F32) * g_ref[t * 32 : t * 32 + 32, :]
            c_ref[pl.ds(pl.multiple_of(b * 128 + m * 32, 32), 32), :] = total
        return carry

    lax.fori_loop(0, 10, contract, 0)
    def along_x(c):
        x = lax.broadcasted_iota(jnp.int32, c.shape, 0) % 16
        up = jnp.where(x == 0, 0.0, pltpu.roll(c, 1, 0))
        down = jnp.where(x == 15, 0.0, pltpu.roll(c, c.shape[0] - 1, 0))
        return 0.5 * c + 0.25 * (up + down)

    def along_y(c, lane):
        left = jnp.where(lane == 0, 0.0, pltpu.roll(c, 1, 1))
        right = jnp.where(lane == 127, 0.0, pltpu.roll(c, 127, 1))
        return 0.5 * c + 0.25 * (left + right)

    lane256 = lax.broadcasted_iota(jnp.int32, (256, 128), 1)
    x256 = lax.broadcasted_iota(jnp.int32, (256, 128), 0) % 16

    def inside(b, carry):
        at = pl.ds(pl.multiple_of(b * 256, 256), 256)
        f_ref[at, :] = along_y(along_x(c_ref[at, :]), lane256)
        return carry

    lax.fori_loop(0, 5, inside, 0)

    for copy in second:
        copy.wait_send()
    remote(xe_buf.at[0], xe_got.at[1], send2.at[0], recv2.at[1], {"tx": west, "ty": ty, "mem": mem}).wait_recv()
    remote(xe_buf.at[1], xe_got.at[0], send2.at[1], recv2.at[0], {"tx": east, "ty": ty, "mem": mem}).wait_recv()
    remote(ce_buf, ce_got, send2.at[2], recv2.at[2], {"tx": tx, "ty": over, "mem": mem}).wait_recv()
    remote(cc_buf.at[0], cc_got.at[1], send2.at[3], recv2.at[4], {"tx": west, "ty": over, "mem": mem}).wait_recv()
    remote(cc_buf.at[1], cc_got.at[0], send2.at[4], recv2.at[3], {"tx": east, "ty": over, "mem": mem}).wait_recv()

    lane80 = lax.broadcasted_iota(jnp.int32, (80, 128), 1)
    hx_ref[0] = along_y(xe_got[0], lane80) * (0.25 * has_west)
    hx_ref[1] = along_y(xe_got[1], lane80) * (0.25 * has_east)
    side = along_x(ce_got[...])
    for v in range(2):
        before = cc_got[0, v : v + 1, :] * (0.25 * has_west)
        behind = cc_got[1, v : v + 1, :] * (0.25 * has_east)
        here = lax.broadcasted_iota(jnp.int32, (32, 128), 0)
        side = side + jnp.where(here == v * 16, before, 0.0) + jnp.where(here == v * 16 + 15, behind, 0.0)
    hy_ref[...] = side * 0.25

    def finish(b, carry):
        at = pl.ds(pl.multiple_of(b * 256, 256), 256)
        side_parts, low, high = [], [], []
        for m in range(8):
            side_parts.append(pltpu.roll(hy_ref[...], lax.rem(edge - (b * 8 + m) + 128, 128), 1))
            for v in range(2):
                low.append(jnp.broadcast_to(hx_ref[0, pl.ds(v * 40 + b * 8 + m, 1), :], (16, 128)))
                high.append(jnp.broadcast_to(hx_ref[1, pl.ds(v * 40 + b * 8 + m, 1), :], (16, 128)))
        f = f_ref[at, :] + jnp.where(lane256 == edge, jnp.concatenate(side_parts, axis=0), 0.0)
        f = f + jnp.where(x256 == 0, jnp.concatenate(low, axis=0), 0.0)
        f = f + jnp.where(x256 == 15, jnp.concatenate(high, axis=0), 0.0)
        out_ref[pl.ds(b * 8, 8)] = f.reshape(8, 32, 128).astype(BF16)
        return carry

    lax.fori_loop(0, 5, finish, 0)

    for copy in first:
        copy.wait_send()

    group(recv_sem.at[0], 0, TILES - 1).wait_send()


def body(obs_value, obs_frac, obs_cell, obs_layer, obs_tile, obs_length, ensemble):
    square = (ROWS, 128)
    dma = pltpu.SemaphoreType.DMA
    out = pl.pallas_call(
        all_kernel,
        out_shape=pltpu.VMEM((40, 32, 128), BF16),
        in_specs=[pl.BlockSpec(memory_space=pltpu.SMEM)] + [pl.BlockSpec(memory_space=pl.ANY)] * 6,
        out_specs=VMEM_SPEC,
        scratch_shapes=[
            pltpu.VMEM(square, F32),
            pltpu.VMEM((2, ROWS * 128), F32),
            pltpu.VMEM(square, jnp.int32),
            pltpu.VMEM(square, jnp.int32),
            pltpu.VMEM(square, jnp.int32),
            pltpu.VMEM(square, F32),
            pltpu.VMEM(square, F32),
            pltpu.VMEM((192, 256), F32),
            pltpu.VMEM((TILES, 6, 128), F32),
            pltpu.VMEM((TILES, 6, 128), F32),
            pltpu.VMEM((272, 192), F32),
            pltpu.VMEM((40, 192, 128), BF16),
            pltpu.VMEM((192, 128), F32),
            pltpu.VMEM((2, 12, 40, 128), F32),
            pltpu.VMEM((192, 128), F32),
            pltpu.VMEM((192, 128), F32),
            pltpu.VMEM((192, 128), F32),
            pltpu.VMEM((12, 128), F32),
            pltpu.VMEM((2, 12, 128), F32),
            pltpu.VMEM((8, 256), F32),
            pltpu.VMEM((2, 8, 256), F32),
            pltpu.VMEM((8, 256), F32),
            pltpu.VMEM((2, 8, 256), F32),
            pltpu.VMEM((192, 128), F32),
            pltpu.VMEM((1280, 128), F32),
            pltpu.VMEM((1280, 128), F32),
            pltpu.VMEM((2, 80, 128), F32),
            pltpu.VMEM((2, 80, 128), F32),
            pltpu.VMEM((32, 128), F32),
            pltpu.VMEM((32, 128), F32),
            pltpu.VMEM((2, 2, 128), F32),
            pltpu.VMEM((2, 2, 128), F32),
            pltpu.VMEM((2, 80, 128), F32),
            pltpu.VMEM((32, 128), F32),
            dma((5,)),
            dma,
            dma,
            dma((16,)),
            dma((7,)),
            dma((7,)),
            dma((5,)),
            dma((5,)),
        ],
        compiler_params=pltpu.CompilerParams(collective_id=0, has_side_effects=True),
    )(
        obs_length,
        obs_value.reshape(square),
        obs_frac,
        obs_cell.reshape(square),
        obs_layer.reshape(square),
        obs_tile.reshape(square),
        ensemble.reshape(40, 192, 128),
    )
    return out.reshape(40, 2, 16, 128)


def solution(mesh):
    placed = (
        P(("tx", "ty", "mem")),
        P(None, ("tx", "ty", "mem")),
        P(("tx", "ty", "mem")),
        P(("tx", "ty", "mem")),
        P(("tx", "ty", "mem")),
        P(("tx", "ty", "mem")),
        P("mem", None, None, "tx", "ty"),
    )
    return jax.shard_map(
        body, mesh=mesh, in_specs=placed, out_specs=P("mem", None, "tx", "ty"), check_vma=False
    )
```

```python
import functools

import jax
import jax.numpy as jnp
from jax import lax
from jax.experimental import pallas as pl
from jax.experimental.pallas import tpu as pltpu
from jax.sharding import PartitionSpec as P

F32 = jnp.float32
BF16 = jnp.bfloat16
MESH_ID = pl.DeviceIdType.MESH
VMEM_SPEC = pl.BlockSpec(memory_space=pltpu.VMEM)
SLOT = 64
TILES = 128
CHUNKS = 3
ROWS = 64
DEAD = 1000.0


def packed_iota(groups, shift):
    a = lax.broadcasted_iota(jnp.int32, (groups, 16, 128), 0)
    b = lax.broadcasted_iota(jnp.int32, (groups, 16, 128), 1)
    return (a * 16 + b + shift).astype(F32).astype(BF16)


def spread_row(row):
    return jnp.broadcast_to(row, (16, 128)).astype(BF16)[None]


def two_parts(x):
    hi = x.astype(BF16).astype(F32)
    return hi, x - hi


def dot_t(a, b):
    return lax.dot_general(a, b, (((1,), (1,)), ((), ())), preferred_element_type=F32)


def dot_n(a, b):
    return lax.dot_general(a, b, (((1,), (0,)), ((), ())), preferred_element_type=F32)


def rank_stage(length, z_own, tile_ref, d_ref, s_ref):
    i = lax.broadcasted_iota(jnp.int32, (128, 256), 0)
    j = lax.broadcasted_iota(jnp.int32, (128, 256), 1)
    before = jnp.where((i < j) | (j >= 128), 1.0, 0.0).astype(BF16)
    tiles_id = lax.broadcasted_iota(jnp.int32, (TILES, 128), 0)
    lane = lax.broadcasted_iota(jnp.int32, (1, 128), 1)
    per = 4

    def step(k, offset):
        for q in range(per):
            r = k * per + q
            t = tile_ref[pl.ds(r, 1), :]
            live = (lane + r * 128) < length
            t = jnp.where(live, t, -1)
            match = tiles_id == t
            both = dot_n(jnp.where(match, 1.0, 0.0).astype(BF16), before)
            rank = jnp.sum(jnp.where(match, both[:, :128] + offset, 0.0), axis=0, keepdims=True)
            offset = offset + both[:, 128:]
            c = jnp.floor(rank * (1.0 / SLOT))
            tf = t.astype(F32)
            t4 = jnp.floor(tf * 0.25)
            z = jnp.floor(t4 * 0.25)
            e = z - z_own.astype(F32) + 6.0
            e = e - 8.0 * jnp.floor(e * 0.125)
            near = jnp.where(e >= 4.0, 1.0, 0.0)
            d = near * 48.0 + c * 16.0 + (e - near * 4.0) * 4.0 + (t4 - z * 4.0)
            d_ref[pl.ds(r, 1), :] = jnp.where(live, d, DEAD)
            s_ref[pl.ds(r, 1), :] = (tf - 4.0 * t4) * SLOT + (rank - c * SLOT)
        return offset

    lax.fori_loop(0, ROWS // per, step, jnp.zeros((TILES, 128), F32))


def pack_stage(near, val_ref, frac_ref, cell_ref, layer_ref, d_ref, s_ref, acc_ref, out_ref):
    d_ids = packed_iota(3, near * 48)
    s_ids = packed_iota(16, 0)
    one = jnp.ones((1, 16, 128), BF16)
    zero = jnp.zeros((1, 16, 128), BF16)
    acc_ref[...] = jnp.zeros_like(acc_ref)
    per = 16

    def step(k, carry):
        rights, highs, lows = [], [], []
        for q in range(per):
            r = k * per + q
            mask = d_ids == spread_row(d_ref[pl.ds(r, 1), :])
            rights.append(jnp.where(s_ids == spread_row(s_ref[pl.ds(r, 1), :]), one, zero).reshape(256, 128))
            v = val_ref[pl.ds(r, 1), :]
            fx = frac_ref[0:1, pl.ds(pl.multiple_of(r * 128, 128), 128)]
            fy = frac_ref[1:2, pl.ds(pl.multiple_of(r * 128, 128), 128)]
            pos = layer_ref[pl.ds(r, 1), :] * 2048 + cell_ref[pl.ds(r, 1), :]
            pos_low = (pos & 255).astype(F32)
            pos_high = pos.astype(F32) - pos_low
            parts = [two_parts(v), (pos_high, pos_low), two_parts(fx), two_parts(fy)]
            for into, p in ((highs, 0), (lows, 1)):
                into.append(
                    jnp.concatenate(
                        [jnp.where(mask, spread_row(w[p]), zero).reshape(48, 128) for w in parts],
                        axis=0,
                    )
                )
        total = jnp.zeros((384, 256), F32)
        for part in (slice(0, per // 2), slice(per // 2, per)):
            left = jnp.concatenate(
                [jnp.concatenate(highs[part], axis=1), jnp.concatenate(lows[part], axis=1)], axis=0
            )
            total = total + dot_t(left, jnp.concatenate(rights[part], axis=1))
        acc_ref[...] += total[:192] + total[192:]
        return carry

    lax.fori_loop(0, ROWS // per, step, 0)
    low = lax.broadcasted_iota(jnp.int32, (16, 128), 1) < SLOT
    for c in range(CHUNKS):
        for col in range(2):
            plain = [acc_ref[w * 48 + c * 16 : w * 48 + c * 16 + 16, col * 128 : col * 128 + 128] for w in range(4)]
            moved = [pltpu.roll(w, SLOT, 1) for w in plain]
            for half in range(2):
                at = (2 * col + half) * 32 + near * 16
                for h in range(2):
                    first, last = (plain[2 * h], moved[2 * h + 1]) if half == 0 else (moved[2 * h], plain[2 * h + 1])
                    out_ref[at : at + 16, 2 * c + h, :] = jnp.where(low, first, last)


def peers(tx, ty):
    z, y, x = tx // 8, (tx // 2) % 4, (tx % 2) * 2 + ty
    z_parts = [((z + dz) % 8) * 8 for dz in range(8)]

    def pair(q):
        px = (x + q) % 4
        py = (y + q // 4) % 4
        return py, px

    return z_parts, pair


def spread_block(r_ref, first, acc_ref):
    lane = lax.broadcasted_iota(jnp.int32, (8, 128), 1)
    low = lane < SLOT
    x_ids = packed_iota(12, 0)
    y_ids = packed_iota(8, 0)
    rim_id = lax.broadcasted_iota(jnp.int32, (16, 128), 0)
    one = jnp.ones((1, 16, 128), BF16)
    zero = jnp.zeros((1, 16, 128), BF16)

    def both(j):
        a = r_ref[pl.ds(first, 8), j, :]
        b = r_ref[pl.ds(first + 8, 8), j, :]
        return jnp.where(low, a, pltpu.roll(b, SLOT, 1)), jnp.where(low, pltpu.roll(a, SLOT, 1), b)

    for c in range(CHUNKS):
        v, pos = both(2 * c)
        fx, fy = both(2 * c + 1)
        key = jnp.floor(pos * (1.0 / 128.0))
        cy = pos - key * 128.0
        v1 = v * fx
        v0 = v * (1.0 - fx)
        gy = 1.0 - fy
        q = [two_parts(u) for u in (v0 * gy, v0 * fy, v1 * gy, v1 * fy)]
        last = cy == 127.0
        rims = [[jnp.where(last, q[1][p], 0.0), jnp.where(last, q[3][p], 0.0)] for p in range(2)]
        rights, lefts = [], [[], []]
        for r in range(8):
            def row(u):
                return u[r : r + 1, :]
            rights.append(jnp.where(x_ids == spread_row(row(key)), one, zero).reshape(192, 128))
            here = spread_row(row(cy))
            m0 = y_ids == here
            m1 = y_ids == spread_row(row(cy) + 1.0)
            for p in range(2):
                pieces = []
                for a in range(2):
                    w0 = spread_row(row(q[2 * a][p]))
                    w1 = spread_row(row(q[2 * a + 1][p]))
                    pieces.append(jnp.where(m0, w0, jnp.where(m1, w1, zero)).reshape(128, 128))
                edge = jnp.where(
                    rim_id == 0,
                    jnp.broadcast_to(row(rims[p][0]), (16, 128)),
                    jnp.where(rim_id == 1, jnp.broadcast_to(row(rims[p][1]), (16, 128)), 0.0),
                ).astype(BF16)
                lefts[p].append(jnp.concatenate(pieces + [edge], axis=0))
        right = jnp.concatenate(rights, axis=1)
        acc_ref[...] += dot_t(jnp.concatenate(lefts[0], axis=1), right) + dot_t(
            jnp.concatenate(lefts[1], axis=1), right
        )


def remote(src, dst, send_sem, recv_sem, where):
    return pltpu.make_async_remote_copy(
        src_ref=src, dst_ref=dst, send_sem=send_sem, recv_sem=recv_sem, device_id=where, device_id_type=MESH_ID
    )


def edge_columns(ens_ref, edge, out_ref):
    k = lax.broadcasted_iota(jnp.int32, (1024, 128), 0)
    col = lax.broadcasted_iota(jnp.int32, (1024, 128), 1)
    total = jnp.zeros((192, 128), F32)
    for g in range(5):
        left = jnp.concatenate([ens_ref[8 * g + m] for m in range(8)], axis=1)
        pick = ((k % 128 == edge) & (k // 128 + 8 * g == col)).astype(F32).astype(BF16)
        total = total + dot_n(left, pick)
    out_ref[...] = total


def edge_rows(ens_ref, out_ref):
    def step(m, carry):
        for k in range(12):
            block = ens_ref[m, k * 16 : k * 16 + 16, :].astype(F32)
            out_ref[0, k, pl.ds(m, 1), :] = block[0:1, :]
            out_ref[1, k, pl.ds(m, 1), :] = block[15:16, :]
        return carry

    lax.fori_loop(0, 40, step, 0)


def all_kernel(
    length_ref, val_hbm, frac_hbm, cell_hbm, layer_hbm, tile_hbm, ens_hbm, out_ref,
    val_ref, frac_ref, cell_ref, layer_ref, tile_ref,
    d_ref, s_ref, acc_ref, sbuf, rbuf, grid_ref, ens_ref, col_ref, rows_ref,
    part_buf, part_got, next_buf, east_buf, east_got, north_buf, north_got, corner_buf, corner_got,
    g_ref, c_ref, f_ref, xe_buf, xe_got, ce_buf, ce_got, cc_buf, cc_got, hx_ref, hy_ref,
    in_sem, ens_sem, send_sem, recv_sem, send1, recv1, send2, recv2,
):
    tx = lax.axis_index("tx")
    ty = lax.axis_index("ty")
    mem = lax.axis_index("mem")
    n_tx = lax.axis_size("tx")
    east = lax.rem(tx + 1, n_tx)
    west = lax.rem(tx + n_tx - 1, n_tx)
    over = 1 - ty
    twin = 1 - mem
    barrier = pltpu.get_barrier_semaphore()

    z_parts, pair = peers(tx, ty)

    def over_peers(act, near):
        steps = (1, 7, 6, 0) if near else (4, 3, 5, 2)

        def some(q, count):
            py, px = pair(q)
            for n in range(count):
                dz = steps[n]
                place = px * 32 + (dz + 6) % 8 * 4 + py
                act(4 - near * 4 + (15 - q) // 4, (15 - q) % 4 * 4 + n, z_parts[dz] + py * 2 + px // 2, px % 2, place)

        def step(i, carry):
            some(15 - i, 4)
            return carry

        lax.fori_loop(0, 15, step, 0)
        some(0, 4 - near)

    def copy_in(src, dst, i):
        copy = pltpu.make_async_copy(src, dst, in_sem.at[i])
        copy.start()
        return copy

    tile_in = copy_in(tile_hbm, tile_ref, 0)
    others_in = [
        copy_in(val_hbm, val_ref, 1),
        copy_in(frac_hbm, frac_ref, 2),
        copy_in(cell_hbm, cell_ref, 3),
        copy_in(layer_hbm, layer_ref, 4),
    ]
    ens_copy = pltpu.make_async_copy(ens_hbm, ens_ref, ens_sem)
    ens_copy.start()

    def greet(k, n, px, py, at):
        pl.semaphore_signal(barrier, inc=1, device_id={"tx": px, "ty": py, "mem": mem}, device_id_type=MESH_ID)

    over_peers(greet, 0)
    over_peers(greet, 1)
    for px, py in ((tx, ty), (west, ty), (tx, over), (west, over)):
        pl.semaphore_signal(barrier, inc=1, device_id={"tx": px, "ty": py, "mem": twin}, device_id_type=MESH_ID)
    tile_in.wait()
    rank_stage(length_ref[0], tx // 8, tile_ref, d_ref, s_ref)
    for copy in others_in:
        copy.wait()
    packing = (val_ref, frac_ref, cell_ref, layer_ref, d_ref, s_ref, acc_ref, sbuf)
    pack_stage(1, *packing)

    pl.semaphore_wait(barrier, TILES - 1 + 4)

    def message(k, n, px, py, at):
        there = {"tx": px, "ty": py, "mem": mem}
        return remote(sbuf.at[at], rbuf.at[k * 16 + n], send_sem, recv_sem.at[k * 2 + n // 15], there)

    def group(sem, first, count):
        at = pl.ds(first, count)
        return remote(sbuf.at[at], rbuf.at[at], send_sem, sem, {"tx": west, "ty": ty, "mem": mem})

    over_peers(lambda *peer: message(*peer).start(), 1)
    pack_stage(0, *packing)
    over_peers(lambda *peer: message(*peer).start(), 0)
    py, px = pair(0)
    rbuf[pl.ds(63, 1)] = sbuf[pl.ds(px * 32 + 24 + py, 1)]
    edge = (1 - ty) * 127

    grid_ref[...] = jnp.zeros_like(grid_ref)

    def gather(k, carry):
        group(recv_sem.at[k * 2], k * 16, 15).wait_recv()

        @pl.when(k != 3)
        def _():
            group(recv_sem.at[k * 2 + 1], k * 16 + 15, 1).wait_recv()

        spread_block(rbuf, k * 16, grid_ref)
        return carry

    lax.fori_loop(0, 8, gather, 0)

    row = lax.broadcasted_iota(jnp.int32, (192, 128), 0)
    x_first = (row % 16) == 0
    lane192 = lax.broadcasted_iota(jnp.int32, (192, 128), 1)
    lane256 = lax.broadcasted_iota(jnp.int32, (8, 256), 1)
    row8 = lax.broadcasted_iota(jnp.int32, (8, 256), 0)
    after = grid_ref[128:256, :].T
    mine = grid_ref[0:128, :].T + jnp.where(x_first, 0.0, pltpu.roll(after, 1, 0))
    part_buf[...] = mine
    next_buf[...] = after
    east_buf[...] = next_buf[pl.ds(15, 12, stride=16), :]
    pad = jnp.zeros((8, 64), F32)
    rim0 = jnp.concatenate([jnp.broadcast_to(grid_ref[256:257, :], (8, 192)), pad], axis=1)
    rim1 = jnp.concatenate([jnp.broadcast_to(grid_ref[257:258, :], (8, 192)), pad], axis=1)
    top = row8 == 0
    first256 = (lane256 % 16) == 0
    north_buf[...] = jnp.where(top, rim0 + jnp.where(first256, 0.0, pltpu.roll(rim1, 1, 1)), 0.0)
    corner_buf[...] = jnp.where(top & first256, pltpu.roll(rim1, 241, 1), 0.0)

    first = [remote(part_buf, part_got, send1.at[0], recv1.at[0], {"tx": tx, "ty": ty, "mem": twin})]
    for j in range(2):
        first.append(remote(east_buf, east_got.at[mem], send1.at[1 + j], recv1.at[1 + mem], {"tx": east, "ty": ty, "mem": j}))
        first.append(remote(north_buf, north_got.at[mem], send1.at[3 + j], recv1.at[3 + mem], {"tx": tx, "ty": over, "mem": j}))
        first.append(remote(corner_buf, corner_got.at[mem], send1.at[5 + j], recv1.at[5 + mem], {"tx": east, "ty": over, "mem": j}))
    for copy in first:
        copy.start()
    ens_copy.wait()
    edge_columns(ens_ref, edge, col_ref)
    edge_rows(ens_ref, rows_ref)
    remote(part_buf, part_got, send1.at[0], recv1.at[0], {"tx": tx, "ty": ty, "mem": twin}).wait_recv()
    for j in range(2):
        remote(east_buf, east_got.at[j], send1.at[1 + j], recv1.at[1 + j], {"tx": east, "ty": ty, "mem": j}).wait_recv()
        remote(north_buf, north_got.at[j], send1.at[3 + j], recv1.at[3 + j], {"tx": tx, "ty": over, "mem": j}).wait_recv()
        remote(corner_buf, corner_got.at[j], send1.at[5 + j], recv1.at[5 + j], {"tx": east, "ty": over, "mem": j}).wait_recv()
    has_west = jnp.where(tx > 0, 1.0, 0.0)
    has_east = jnp.where(tx < n_tx - 1, 1.0, 0.0)
    has_south = jnp.where(ty > 0, 1.0, 0.0)
    rims = (north_got[0] + north_got[1] + (corner_got[0] + corner_got[1]) * has_west) * has_south
    rims = jnp.concatenate([rims, jnp.zeros((120, 256), F32)], axis=0).T
    wall = (east_got[0] + east_got[1]) * has_west
    wall = jnp.broadcast_to(wall[:, None, :], (12, 16, 128)).reshape(192, 128)
    g = part_buf[...] + part_got[...] + rims[0:192, :] + jnp.where(x_first, wall, 0.0)
    g_ref[...] = g
    for n in range(2):
        for v in range(2):
            total = jnp.zeros((40, 128), F32)
            for t in range(6):
                at = (t * 2 + v) * 16 + 15 * n
                total = total + rows_ref[n, t * 2 + v] * g[at : at + 1, :]
            xe_buf[n, v * 40 : v * 40 + 40, :] = total
    second = [
        remote(xe_buf.at[0], xe_got.at[1], send2.at[0], recv2.at[1], {"tx": west, "ty": ty, "mem": mem}),
        remote(xe_buf.at[1], xe_got.at[0], send2.at[1], recv2.at[0], {"tx": east, "ty": ty, "mem": mem}),
        remote(ce_buf, ce_got, send2.at[2], recv2.at[2], {"tx": tx, "ty": over, "mem": mem}),
        remote(cc_buf.at[0], cc_got.at[1], send2.at[3], recv2.at[4], {"tx": west, "ty": over, "mem": mem}),
        remote(cc_buf.at[1], cc_got.at[0], send2.at[4], recv2.at[3], {"tx": east, "ty": over, "mem": mem}),
    ]
    second[0].start()
    second[1].start()
    gcol = jnp.sum(jnp.where(lane192 == edge, g, 0.0), axis=1, keepdims=True)
    ce = jnp.zeros((32, 128), F32)
    for t in range(6):
        ce = ce + col_ref[t * 32 : t * 32 + 32, :] * gcol[t * 32 : t * 32 + 32, :]
    ce_buf[...] = ce
    for v in range(2):
        cc_buf[0, v : v + 1, :] = ce[v * 16 : v * 16 + 1, :]
        cc_buf[1, v : v + 1, :] = ce[v * 16 + 15 : v * 16 + 16, :]

    for copy in second[2:]:
        copy.start()

    def contract(b, carry):
        for m in range(4):
            total = jnp.zeros((32, 128), F32)
            for t in range(6):
                total = total + ens_ref[b * 4 + m, t * 32 : t * 32 + 32, :].astype(F32) * g_ref[t * 32 : t * 32 + 32, :]
            c_ref[pl.ds(pl.multiple_of(b * 128 + m * 32, 32), 32), :] = total
        return carry

    lax.fori_loop(0, 10, contract, 0)
    def along_x(c):
        x = lax.broadcasted_iota(jnp.int32, c.shape, 0) % 16
        up = jnp.where(x == 0, 0.0, pltpu.roll(c, 1, 0))
        down = jnp.where(x == 15, 0.0, pltpu.roll(c, c.shape[0] - 1, 0))
        return 0.5 * c + 0.25 * (up + down)

    def along_y(c, lane):
        left = jnp.where(lane == 0, 0.0, pltpu.roll(c, 1, 1))
        right = jnp.where(lane == 127, 0.0, pltpu.roll(c, 127, 1))
        return 0.5 * c + 0.25 * (left + right)

    lane256 = lax.broadcasted_iota(jnp.int32, (256, 128), 1)
    x256 = lax.broadcasted_iota(jnp.int32, (256, 128), 0) % 16

    def inside(b, carry):
        at = pl.ds(pl.multiple_of(b * 256, 256), 256)
        f_ref[at, :] = along_y(along_x(c_ref[at, :]), lane256)
        return carry

    lax.fori_loop(0, 5, inside, 0)

    for copy in second:
        copy.wait_send()
    remote(xe_buf.at[0], xe_got.at[1], send2.at[0], recv2.at[1], {"tx": west, "ty": ty, "mem": mem}).wait_recv()
    remote(xe_buf.at[1], xe_got.at[0], send2.at[1], recv2.at[0], {"tx": east, "ty": ty, "mem": mem}).wait_recv()
    remote(ce_buf, ce_got, send2.at[2], recv2.at[2], {"tx": tx, "ty": over, "mem": mem}).wait_recv()
    remote(cc_buf.at[0], cc_got.at[1], send2.at[3], recv2.at[4], {"tx": west, "ty": over, "mem": mem}).wait_recv()
    remote(cc_buf.at[1], cc_got.at[0], send2.at[4], recv2.at[3], {"tx": east, "ty": over, "mem": mem}).wait_recv()

    lane80 = lax.broadcasted_iota(jnp.int32, (80, 128), 1)
    hx_ref[0] = along_y(xe_got[0], lane80) * (0.25 * has_west)
    hx_ref[1] = along_y(xe_got[1], lane80) * (0.25 * has_east)
    side = along_x(ce_got[...])
    for v in range(2):
        before = cc_got[0, v : v + 1, :] * (0.25 * has_west)
        behind = cc_got[1, v : v + 1, :] * (0.25 * has_east)
        here = lax.broadcasted_iota(jnp.int32, (32, 128), 0)
        side = side + jnp.where(here == v * 16, before, 0.0) + jnp.where(here == v * 16 + 15, behind, 0.0)
    hy_ref[...] = side * 0.25

    def finish(b, carry):
        at = pl.ds(pl.multiple_of(b * 256, 256), 256)
        side_parts, low, high = [], [], []
        for m in range(8):
            side_parts.append(pltpu.roll(hy_ref[...], lax.rem(edge - (b * 8 + m) + 128, 128), 1))
            for v in range(2):
                low.append(jnp.broadcast_to(hx_ref[0, pl.ds(v * 40 + b * 8 + m, 1), :], (16, 128)))
                high.append(jnp.broadcast_to(hx_ref[1, pl.ds(v * 40 + b * 8 + m, 1), :], (16, 128)))
        f = f_ref[at, :] + jnp.where(lane256 == edge, jnp.concatenate(side_parts, axis=0), 0.0)
        f = f + jnp.where(x256 == 0, jnp.concatenate(low, axis=0), 0.0)
        f = f + jnp.where(x256 == 15, jnp.concatenate(high, axis=0), 0.0)
        out_ref[pl.ds(b * 8, 8)] = f.reshape(8, 32, 128).astype(BF16)
        return carry

    lax.fori_loop(0, 5, finish, 0)

    for copy in first:
        copy.wait_send()

    group(recv_sem.at[0], 0, TILES - 1).wait_send()


def body(obs_value, obs_frac, obs_cell, obs_layer, obs_tile, obs_length, ensemble):
    square = (ROWS, 128)
    dma = pltpu.SemaphoreType.DMA
    out = pl.pallas_call(
        all_kernel,
        out_shape=pltpu.VMEM((40, 32, 128), BF16),
        in_specs=[pl.BlockSpec(memory_space=pltpu.SMEM)] + [pl.BlockSpec(memory_space=pl.ANY)] * 6,
        out_specs=VMEM_SPEC,
        scratch_shapes=[
            pltpu.VMEM(square, F32),
            pltpu.VMEM((2, ROWS * 128), F32),
            pltpu.VMEM(square, jnp.int32),
            pltpu.VMEM(square, jnp.int32),
            pltpu.VMEM(square, jnp.int32),
            pltpu.VMEM(square, F32),
            pltpu.VMEM(square, F32),
            pltpu.VMEM((192, 256), F32),
            pltpu.VMEM((TILES, 6, 128), F32),
            pltpu.VMEM((TILES, 6, 128), F32),
            pltpu.VMEM((272, 192), F32),
            pltpu.VMEM((40, 192, 128), BF16),
            pltpu.VMEM((192, 128), F32),
            pltpu.VMEM((2, 12, 40, 128), F32),
            pltpu.VMEM((192, 128), F32),
            pltpu.VMEM((192, 128), F32),
            pltpu.VMEM((192, 128), F32),
            pltpu.VMEM((12, 128), F32),
            pltpu.VMEM((2, 12, 128), F32),
            pltpu.VMEM((8, 256), F32),
            pltpu.VMEM((2, 8, 256), F32),
            pltpu.VMEM((8, 256), F32),
            pltpu.VMEM((2, 8, 256), F32),
            pltpu.VMEM((192, 128), F32),
            pltpu.VMEM((1280, 128), F32),
            pltpu.VMEM((1280, 128), F32),
            pltpu.VMEM((2, 80, 128), F32),
            pltpu.VMEM((2, 80, 128), F32),
            pltpu.VMEM((32, 128), F32),
            pltpu.VMEM((32, 128), F32),
            pltpu.VMEM((2, 2, 128), F32),
            pltpu.VMEM((2, 2, 128), F32),
            pltpu.VMEM((2, 80, 128), F32),
            pltpu.VMEM((32, 128), F32),
            dma((5,)),
            dma,
            dma,
            dma((16,)),
            dma((7,)),
            dma((7,)),
            dma((5,)),
            dma((5,)),
        ],
        compiler_params=pltpu.CompilerParams(collective_id=0, has_side_effects=True),
    )(
        obs_length,
        obs_value.reshape(square),
        obs_frac,
        obs_cell.reshape(square),
        obs_layer.reshape(square),
        obs_tile.reshape(square),
        ensemble.reshape(40, 192, 128),
    )
    return out.reshape(40, 2, 16, 128)


def solution(mesh):
    placed = (
        P(("tx", "ty", "mem")),
        P(None, ("tx", "ty", "mem")),
        P(("tx", "ty", "mem")),
        P(("tx", "ty", "mem")),
        P(("tx", "ty", "mem")),
        P(("tx", "ty", "mem")),
        P("mem", None, None, "tx", "ty"),
    )
    return jax.shard_map(
        body, mesh=mesh, in_specs=placed, out_specs=P("mem", None, "tx", "ty"), check_vma=False
    )
```

```python
import functools

import jax
import jax.numpy as jnp
from jax import lax
from jax.experimental import pallas as pl
from jax.experimental.pallas import tpu as pltpu
from jax.sharding import PartitionSpec as P

F32 = jnp.float32
BF16 = jnp.bfloat16
MESH_ID = pl.DeviceIdType.MESH
VMEM_SPEC = pl.BlockSpec(memory_space=pltpu.VMEM)
SLOT = 64
TILES = 128
CHUNKS = 3
ROWS = 64
DEAD = 1000.0


def packed_iota(groups, shift):
    a = lax.broadcasted_iota(jnp.int32, (groups, 16, 128), 0)
    b = lax.broadcasted_iota(jnp.int32, (groups, 16, 128), 1)
    return (a * 16 + b + shift).astype(F32).astype(BF16)


def spread_row(row):
    return jnp.broadcast_to(row, (16, 128)).astype(BF16)[None]


def two_parts(x):
    hi = x.astype(BF16).astype(F32)
    return hi, x - hi


def dot_t(a, b):
    return lax.dot_general(a, b, (((1,), (1,)), ((), ())), preferred_element_type=F32)


def dot_n(a, b):
    return lax.dot_general(a, b, (((1,), (0,)), ((), ())), preferred_element_type=F32)


def rank_stage(length, z_own, tile_ref, d_ref, s_ref):
    i = lax.broadcasted_iota(jnp.int32, (128, 256), 0)
    j = lax.broadcasted_iota(jnp.int32, (128, 256), 1)
    before = jnp.where((i < j) | (j >= 128), 1.0, 0.0).astype(BF16)
    tiles_id = lax.broadcasted_iota(jnp.int32, (TILES, 128), 0)
    lane = lax.broadcasted_iota(jnp.int32, (1, 128), 1)
    per = 8

    def step(k, offset):
        for q in range(per):
            r = k * per + q
            t = tile_ref[pl.ds(r, 1), :]
            live = (lane + r * 128) < length
            t = jnp.where(live, t, -1)
            match = tiles_id == t
            both = dot_n(jnp.where(match, 1.0, 0.0).astype(BF16), before)
            rank = jnp.sum(jnp.where(match, both[:, :128] + offset, 0.0), axis=0, keepdims=True)
            offset = offset + both[:, 128:]
            c = jnp.floor(rank * (1.0 / SLOT))
            tf = t.astype(F32)
            t4 = jnp.floor(tf * 0.25)
            z = jnp.floor(t4 * 0.25)
            e = z - z_own.astype(F32) + 6.0
            e = e - 8.0 * jnp.floor(e * 0.125)
            near = jnp.where(e >= 4.0, 1.0, 0.0)
            d = near * 48.0 + c * 16.0 + (e - near * 4.0) * 4.0 + (t4 - z * 4.0)
            d_ref[pl.ds(r, 1), :] = jnp.where(live, d, DEAD)
            s_ref[pl.ds(r, 1), :] = (tf - 4.0 * t4) * SLOT + (rank - c * SLOT)
        return offset

    lax.fori_loop(0, ROWS // per, step, jnp.zeros((TILES, 128), F32))


def pack_stage(near, val_ref, frac_ref, cell_ref, layer_ref, d_ref, s_ref, acc_ref, out_ref):
    d_ids = packed_iota(3, near * 48)
    s_ids = packed_iota(16, 0)
    one = jnp.ones((1, 16, 128), BF16)
    zero = jnp.zeros((1, 16, 128), BF16)
    acc_ref[...] = jnp.zeros_like(acc_ref)
    per = 16

    def step(k, carry):
        rights, highs, lows = [], [], []
        for q in range(per):
            r = k * per + q
            mask = d_ids == spread_row(d_ref[pl.ds(r, 1), :])
            rights.append(jnp.where(s_ids == spread_row(s_ref[pl.ds(r, 1), :]), one, zero).reshape(256, 128))
            v = val_ref[pl.ds(r, 1), :]
            fx = frac_ref[0:1, pl.ds(pl.multiple_of(r * 128, 128), 128)]
            fy = frac_ref[1:2, pl.ds(pl.multiple_of(r * 128, 128), 128)]
            pos = layer_ref[pl.ds(r, 1), :] * 2048 + cell_ref[pl.ds(r, 1), :]
            pos_low = (pos & 255).astype(F32)
            pos_high = pos.astype(F32) - pos_low
            parts = [two_parts(v), (pos_high, pos_low), two_parts(fx), two_parts(fy)]
            for into, p in ((highs, 0), (lows, 1)):
                into.append(
                    jnp.concatenate(
                        [jnp.where(mask, spread_row(w[p]), zero).reshape(48, 128) for w in parts],
                        axis=0,
                    )
                )
        total = jnp.zeros((384, 256), F32)
        for part in (slice(0, per // 2), slice(per // 2, per)):
            left = jnp.concatenate(
                [jnp.concatenate(highs[part], axis=1), jnp.concatenate(lows[part], axis=1)], axis=0
            )
            total = total + dot_t(left, jnp.concatenate(rights[part], axis=1))
        acc_ref[...] += total[:192] + total[192:]
        return carry

    lax.fori_loop(0, ROWS // per, step, 0)
    low = lax.broadcasted_iota(jnp.int32, (16, 128), 1) < SLOT
    for c in range(CHUNKS):
        for col in range(2):
            plain = [acc_ref[w * 48 + c * 16 : w * 48 + c * 16 + 16, col * 128 : col * 128 + 128] for w in range(4)]
            moved = [pltpu.roll(w, SLOT, 1) for w in plain]
            for half in range(2):
                at = (2 * col + half) * 32 + near * 16
                for h in range(2):
                    first, last = (plain[2 * h], moved[2 * h + 1]) if half == 0 else (moved[2 * h], plain[2 * h + 1])
                    out_ref[at : at + 16, 2 * c + h, :] = jnp.where(low, first, last)


def peers(tx, ty):
    z, y, x = tx // 8, (tx // 2) % 4, (tx % 2) * 2 + ty
    z_parts = [((z + dz) % 8) * 8 for dz in range(8)]

    def pair(q):
        px = (x + q) % 4
        py = (y + q // 4) % 4
        return py, px

    return z_parts, pair


def spread_block(r_ref, first, acc_ref):
    lane = lax.broadcasted_iota(jnp.int32, (8, 128), 1)
    low = lane < SLOT
    x_ids = packed_iota(12, 0)
    y_ids = packed_iota(8, 0)
    rim_id = lax.broadcasted_iota(jnp.int32, (16, 128), 0)
    one = jnp.ones((1, 16, 128), BF16)
    zero = jnp.zeros((1, 16, 128), BF16)

    def both(j):
        a = r_ref[pl.ds(first, 8), j, :]
        b = r_ref[pl.ds(first + 8, 8), j, :]
        return jnp.where(low, a, pltpu.roll(b, SLOT, 1)), jnp.where(low, pltpu.roll(a, SLOT, 1), b)

    for c in range(CHUNKS):
        v, pos = both(2 * c)
        fx, fy = both(2 * c + 1)
        key = jnp.floor(pos * (1.0 / 128.0))
        cy = pos - key * 128.0
        v1 = v * fx
        v0 = v * (1.0 - fx)
        gy = 1.0 - fy
        q = [two_parts(u) for u in (v0 * gy, v0 * fy, v1 * gy, v1 * fy)]
        last = cy == 127.0
        rims = [[jnp.where(last, q[1][p], 0.0), jnp.where(last, q[3][p], 0.0)] for p in range(2)]
        rights, lefts = [], [[], []]
        for r in range(8):
            def row(u):
                return u[r : r + 1, :]
            rights.append(jnp.where(x_ids == spread_row(row(key)), one, zero).reshape(192, 128))
            here = spread_row(row(cy))
            m0 = y_ids == here
            m1 = y_ids == spread_row(row(cy) + 1.0)
            for p in range(2):
                pieces = []
                for a in range(2):
                    w0 = spread_row(row(q[2 * a][p]))
                    w1 = spread_row(row(q[2 * a + 1][p]))
                    pieces.append(jnp.where(m0, w0, jnp.where(m1, w1, zero)).reshape(128, 128))
                edge = jnp.where(
                    rim_id == 0,
                    jnp.broadcast_to(row(rims[p][0]), (16, 128)),
                    jnp.where(rim_id == 1, jnp.broadcast_to(row(rims[p][1]), (16, 128)), 0.0),
                ).astype(BF16)
                lefts[p].append(jnp.concatenate(pieces + [edge], axis=0))
        right = jnp.concatenate(rights, axis=1)
        acc_ref[...] += dot_t(jnp.concatenate(lefts[0], axis=1), right) + dot_t(
            jnp.concatenate(lefts[1], axis=1), right
        )


def remote(src, dst, send_sem, recv_sem, where):
    return pltpu.make_async_remote_copy(
        src_ref=src, dst_ref=dst, send_sem=send_sem, recv_sem=recv_sem, device_id=where, device_id_type=MESH_ID
    )


def edge_columns(ens_ref, edge, out_ref):
    k = lax.broadcasted_iota(jnp.int32, (1024, 128), 0)
    col = lax.broadcasted_iota(jnp.int32, (1024, 128), 1)
    total = jnp.zeros((192, 128), F32)
    for g in range(5):
        left = jnp.concatenate([ens_ref[8 * g + m] for m in range(8)], axis=1)
        pick = ((k % 128 == edge) & (k // 128 + 8 * g == col)).astype(F32).astype(BF16)
        total = total + dot_n(left, pick)
    out_ref[...] = total


def edge_rows(ens_ref, out_ref):
    def step(m, carry):
        for k in range(12):
            block = ens_ref[m, k * 16 : k * 16 + 16, :].astype(F32)
            out_ref[0, k, pl.ds(m, 1), :] = block[0:1, :]
            out_ref[1, k, pl.ds(m, 1), :] = block[15:16, :]
        return carry

    lax.fori_loop(0, 40, step, 0)


def all_kernel(
    length_ref, val_hbm, frac_hbm, cell_hbm, layer_hbm, tile_hbm, ens_hbm, out_ref,
    val_ref, frac_ref, cell_ref, layer_ref, tile_ref,
    d_ref, s_ref, acc_ref, sbuf, rbuf, grid_ref, ens_ref, col_ref, rows_ref,
    part_buf, part_got, east_buf, east_got, north_buf, north_got, corner_buf, corner_got,
    g_ref, c_ref, f_ref, xe_buf, xe_got, ce_buf, ce_got, cc_buf, cc_got, hx_ref, hy_ref,
    in_sem, ens_sem, send_sem, recv_sem, send1, recv1, send2, recv2,
):
    tx = lax.axis_index("tx")
    ty = lax.axis_index("ty")
    mem = lax.axis_index("mem")
    n_tx = lax.axis_size("tx")
    east = lax.rem(tx + 1, n_tx)
    west = lax.rem(tx + n_tx - 1, n_tx)
    over = 1 - ty
    twin = 1 - mem
    barrier = pltpu.get_barrier_semaphore()

    z_parts, pair = peers(tx, ty)

    def over_peers(act, near):
        steps = (1, 7, 6, 0) if near else (4, 3, 5, 2)

        def some(q, count):
            py, px = pair(q)
            for n in range(count):
                dz = steps[n]
                place = px * 32 + (dz + 6) % 8 * 4 + py
                act(4 - near * 4 + (15 - q) // 4, (15 - q) % 4 * 4 + n, z_parts[dz] + py * 2 + px // 2, px % 2, place)

        def step(i, carry):
            some(15 - i, 4)
            return carry

        lax.fori_loop(0, 15, step, 0)
        some(0, 4 - near)

    def copy_in(src, dst, i):
        copy = pltpu.make_async_copy(src, dst, in_sem.at[i])
        copy.start()
        return copy

    tile_in = copy_in(tile_hbm, tile_ref, 0)
    others_in = [
        copy_in(val_hbm, val_ref, 1),
        copy_in(frac_hbm, frac_ref, 2),
        copy_in(cell_hbm, cell_ref, 3),
        copy_in(layer_hbm, layer_ref, 4),
    ]
    ens_copy = pltpu.make_async_copy(ens_hbm, ens_ref, ens_sem)
    ens_copy.start()

    def greet(k, n, px, py, at):
        pl.semaphore_signal(barrier, inc=1, device_id={"tx": px, "ty": py, "mem": mem}, device_id_type=MESH_ID)

    over_peers(greet, 0)
    over_peers(greet, 1)
    for px, py in ((tx, ty), (west, ty), (tx, over), (west, over)):
        pl.semaphore_signal(barrier, inc=1, device_id={"tx": px, "ty": py, "mem": twin}, device_id_type=MESH_ID)
    tile_in.wait()
    rank_stage(length_ref[0], tx // 8, tile_ref, d_ref, s_ref)
    for copy in others_in:
        copy.wait()
    packing = (val_ref, frac_ref, cell_ref, layer_ref, d_ref, s_ref, acc_ref, sbuf)
    pack_stage(1, *packing)

    pl.semaphore_wait(barrier, TILES - 1 + 4)

    def message(k, n, px, py, at):
        there = {"tx": px, "ty": py, "mem": mem}
        return remote(sbuf.at[at], rbuf.at[k * 16 + n], send_sem, recv_sem.at[k * 2 + n // 15], there)

    def group(sem, first, count):
        at = pl.ds(first, count)
        return remote(sbuf.at[at], rbuf.at[at], send_sem, sem, {"tx": west, "ty": ty, "mem": mem})

    over_peers(lambda *peer: message(*peer).start(), 1)
    pack_stage(0, *packing)
    over_peers(lambda *peer: message(*peer).start(), 0)
    py, px = pair(0)
    rbuf[pl.ds(63, 1)] = sbuf[pl.ds(px * 32 + 24 + py, 1)]
    edge = (1 - ty) * 127

    grid_ref[...] = jnp.zeros_like(grid_ref)

    def gather(k, carry):
        group(recv_sem.at[k * 2], k * 16, 15).wait_recv()

        @pl.when(k != 3)
        def _():
            group(recv_sem.at[k * 2 + 1], k * 16 + 15, 1).wait_recv()

        spread_block(rbuf, k * 16, grid_ref)
        return carry

    lax.fori_loop(0, 8, gather, 0)

    row = lax.broadcasted_iota(jnp.int32, (192, 128), 0)
    x_first = (row % 16) == 0
    lane192 = lax.broadcasted_iota(jnp.int32, (192, 128), 1)
    lane256 = lax.broadcasted_iota(jnp.int32, (8, 256), 1)
    row8 = lax.broadcasted_iota(jnp.int32, (8, 256), 0)
    after = grid_ref[128:256, :].T
    mine = grid_ref[0:128, :].T + jnp.where(x_first, 0.0, pltpu.roll(after, 1, 0))
    part_buf[...] = mine
    for k in range(12):
        east_buf[k : k + 1, :] = after[k * 16 + 15 : k * 16 + 16, :]
    pad = jnp.zeros((8, 64), F32)
    rim0 = jnp.concatenate([jnp.broadcast_to(grid_ref[256:257, :], (8, 192)), pad], axis=1)
    rim1 = jnp.concatenate([jnp.broadcast_to(grid_ref[257:258, :], (8, 192)), pad], axis=1)
    top = row8 == 0
    first256 = (lane256 % 16) == 0
    north_buf[...] = jnp.where(top, rim0 + jnp.where(first256, 0.0, pltpu.roll(rim1, 1, 1)), 0.0)
    corner_buf[...] = jnp.where(top & first256, pltpu.roll(rim1, 241, 1), 0.0)

    first = [remote(part_buf, part_got, send1.at[0], recv1.at[0], {"tx": tx, "ty": ty, "mem": twin})]
    for j in range(2):
        first.append(remote(east_buf, east_got.at[mem], send1.at[1 + j], recv1.at[1 + mem], {"tx": east, "ty": ty, "mem": j}))
        first.append(remote(north_buf, north_got.at[mem], send1.at[3 + j], recv1.at[3 + mem], {"tx": tx, "ty": over, "mem": j}))
        first.append(remote(corner_buf, corner_got.at[mem], send1.at[5 + j], recv1.at[5 + mem], {"tx": east, "ty": over, "mem": j}))
    for copy in first[1:] + first[:1]:
        copy.start()
    ens_copy.wait()
    edge_columns(ens_ref, edge, col_ref)
    edge_rows(ens_ref, rows_ref)
    remote(part_buf, part_got, send1.at[0], recv1.at[0], {"tx": tx, "ty": ty, "mem": twin}).wait_recv()
    for j in range(2):
        remote(east_buf, east_got.at[j], send1.at[1 + j], recv1.at[1 + j], {"tx": east, "ty": ty, "mem": j}).wait_recv()
        remote(north_buf, north_got.at[j], send1.at[3 + j], recv1.at[3 + j], {"tx": tx, "ty": over, "mem": j}).wait_recv()
        remote(corner_buf, corner_got.at[j], send1.at[5 + j], recv1.at[5 + j], {"tx": east, "ty": over, "mem": j}).wait_recv()
    has_west = jnp.where(tx > 0, 1.0, 0.0)
    has_east = jnp.where(tx < n_tx - 1, 1.0, 0.0)
    has_south = jnp.where(ty > 0, 1.0, 0.0)
    rims = (north_got[0] + north_got[1] + (corner_got[0] + corner_got[1]) * has_west) * has_south
    rims = jnp.concatenate([rims, jnp.zeros((120, 256), F32)], axis=0).T
    wall = (east_got[0] + east_got[1]) * has_west
    wall = jnp.broadcast_to(wall[:, None, :], (12, 16, 128)).reshape(192, 128)
    g = part_buf[...] + part_got[...] + rims[0:192, :] + jnp.where(x_first, wall, 0.0)
    g_ref[...] = g
    for n in range(2):
        for v in range(2):
            total = jnp.zeros((40, 128), F32)
            for t in range(6):
                at = (t * 2 + v) * 16 + 15 * n
                total = total + rows_ref[n, t * 2 + v] * g[at : at + 1, :]
            xe_buf[n, v * 40 : v * 40 + 40, :] = total
    second = [
        remote(xe_buf.at[0], xe_got.at[1], send2.at[0], recv2.at[1], {"tx": west, "ty": ty, "mem": mem}),
        remote(xe_buf.at[1], xe_got.at[0], send2.at[1], recv2.at[0], {"tx": east, "ty": ty, "mem": mem}),
        remote(ce_buf, ce_got, send2.at[2], recv2.at[2], {"tx": tx, "ty": over, "mem": mem}),
        remote(cc_buf.at[0], cc_got.at[1], send2.at[3], recv2.at[4], {"tx": west, "ty": over, "mem": mem}),
        remote(cc_buf.at[1], cc_got.at[0], send2.at[4], recv2.at[3], {"tx": east, "ty": over, "mem": mem}),
    ]
    second[0].start()
    second[1].start()
    gcol = jnp.sum(jnp.where(lane192 == edge, g, 0.0), axis=1, keepdims=True)
    ce = jnp.zeros((32, 128), F32)
    for t in range(6):
        ce = ce + col_ref[t * 32 : t * 32 + 32, :] * gcol[t * 32 : t * 32 + 32, :]
    ce_buf[...] = ce
    for v in range(2):
        cc_buf[0, v : v + 1, :] = ce[v * 16 : v * 16 + 1, :]
        cc_buf[1, v : v + 1, :] = ce[v * 16 + 15 : v * 16 + 16, :]

    for copy in second[2:]:
        copy.start()

    def contract(b, carry):
        for m in range(4):
            total = jnp.zeros((32, 128), F32)
            for t in range(6):
                total = total + ens_ref[b * 4 + m, t * 32 : t * 32 + 32, :].astype(F32) * g_ref[t * 32 : t * 32 + 32, :]
            c_ref[pl.ds(pl.multiple_of(b * 128 + m * 32, 32), 32), :] = total
        return carry

    lax.fori_loop(0, 10, contract, 0)
    def along_x(c):
        x = lax.broadcasted_iota(jnp.int32, c.shape, 0) % 16
        up = jnp.where(x == 0, 0.0, pltpu.roll(c, 1, 0))
        down = jnp.where(x == 15, 0.0, pltpu.roll(c, c.shape[0] - 1, 0))
        return 0.5 * c + 0.25 * (up + down)

    def along_y(c, lane):
        left = jnp.where(lane == 0, 0.0, pltpu.roll(c, 1, 1))
        right = jnp.where(lane == 127, 0.0, pltpu.roll(c, 127, 1))
        return 0.5 * c + 0.25 * (left + right)

    lane256 = lax.broadcasted_iota(jnp.int32, (256, 128), 1)
    x256 = lax.broadcasted_iota(jnp.int32, (256, 128), 0) % 16

    def inside(b, carry):
        at = pl.ds(pl.multiple_of(b * 256, 256), 256)
        f_ref[at, :] = along_y(along_x(c_ref[at, :]), lane256)
        return carry

    lax.fori_loop(0, 5, inside, 0)

    for copy in second:
        copy.wait_send()
    remote(xe_buf.at[0], xe_got.at[1], send2.at[0], recv2.at[1], {"tx": west, "ty": ty, "mem": mem}).wait_recv()
    remote(xe_buf.at[1], xe_got.at[0], send2.at[1], recv2.at[0], {"tx": east, "ty": ty, "mem": mem}).wait_recv()
    remote(ce_buf, ce_got, send2.at[2], recv2.at[2], {"tx": tx, "ty": over, "mem": mem}).wait_recv()
    remote(cc_buf.at[0], cc_got.at[1], send2.at[3], recv2.at[4], {"tx": west, "ty": over, "mem": mem}).wait_recv()
    remote(cc_buf.at[1], cc_got.at[0], send2.at[4], recv2.at[3], {"tx": east, "ty": over, "mem": mem}).wait_recv()

    lane80 = lax.broadcasted_iota(jnp.int32, (80, 128), 1)
    hx_ref[0] = along_y(xe_got[0], lane80) * (0.25 * has_west)
    hx_ref[1] = along_y(xe_got[1], lane80) * (0.25 * has_east)
    side = along_x(ce_got[...])
    for v in range(2):
        before = cc_got[0, v : v + 1, :] * (0.25 * has_west)
        behind = cc_got[1, v : v + 1, :] * (0.25 * has_east)
        here = lax.broadcasted_iota(jnp.int32, (32, 128), 0)
        side = side + jnp.where(here == v * 16, before, 0.0) + jnp.where(here == v * 16 + 15, behind, 0.0)
    hy_ref[...] = side * 0.25

    def finish(b, carry):
        at = pl.ds(pl.multiple_of(b * 256, 256), 256)
        side_parts, low, high = [], [], []
        for m in range(8):
            side_parts.append(pltpu.roll(hy_ref[...], lax.rem(edge - (b * 8 + m) + 128, 128), 1))
            for v in range(2):
                low.append(jnp.broadcast_to(hx_ref[0, pl.ds(v * 40 + b * 8 + m, 1), :], (16, 128)))
                high.append(jnp.broadcast_to(hx_ref[1, pl.ds(v * 40 + b * 8 + m, 1), :], (16, 128)))
        f = f_ref[at, :] + jnp.where(lane256 == edge, jnp.concatenate(side_parts, axis=0), 0.0)
        f = f + jnp.where(x256 == 0, jnp.concatenate(low, axis=0), 0.0)
        f = f + jnp.where(x256 == 15, jnp.concatenate(high, axis=0), 0.0)
        out_ref[pl.ds(b * 8, 8)] = f.reshape(8, 32, 128).astype(BF16)
        return carry

    lax.fori_loop(0, 5, finish, 0)

    for copy in first:
        copy.wait_send()

    group(recv_sem.at[0], 0, TILES - 1).wait_send()


def body(obs_value, obs_frac, obs_cell, obs_layer, obs_tile, obs_length, ensemble):
    square = (ROWS, 128)
    dma = pltpu.SemaphoreType.DMA
    out = pl.pallas_call(
        all_kernel,
        out_shape=pltpu.VMEM((40, 32, 128), BF16),
        in_specs=[pl.BlockSpec(memory_space=pltpu.SMEM)] + [pl.BlockSpec(memory_space=pl.ANY)] * 6,
        out_specs=VMEM_SPEC,
        scratch_shapes=[
            pltpu.VMEM(square, F32),
            pltpu.VMEM((2, ROWS * 128), F32),
            pltpu.VMEM(square, jnp.int32),
            pltpu.VMEM(square, jnp.int32),
            pltpu.VMEM(square, jnp.int32),
            pltpu.VMEM(square, F32),
            pltpu.VMEM(square, F32),
            pltpu.VMEM((192, 256), F32),
            pltpu.VMEM((TILES, 6, 128), F32),
            pltpu.VMEM((TILES, 6, 128), F32),
            pltpu.VMEM((272, 192), F32),
            pltpu.VMEM((40, 192, 128), BF16),
            pltpu.VMEM((192, 128), F32),
            pltpu.VMEM((2, 12, 40, 128), F32),
            pltpu.VMEM((192, 128), F32),
            pltpu.VMEM((192, 128), F32),
            pltpu.VMEM((12, 128), F32),
            pltpu.VMEM((2, 12, 128), F32),
            pltpu.VMEM((8, 256), F32),
            pltpu.VMEM((2, 8, 256), F32),
            pltpu.VMEM((8, 256), F32),
            pltpu.VMEM((2, 8, 256), F32),
            pltpu.VMEM((192, 128), F32),
            pltpu.VMEM((1280, 128), F32),
            pltpu.VMEM((1280, 128), F32),
            pltpu.VMEM((2, 80, 128), F32),
            pltpu.VMEM((2, 80, 128), F32),
            pltpu.VMEM((32, 128), F32),
            pltpu.VMEM((32, 128), F32),
            pltpu.VMEM((2, 2, 128), F32),
            pltpu.VMEM((2, 2, 128), F32),
            pltpu.VMEM((2, 80, 128), F32),
            pltpu.VMEM((32, 128), F32),
            dma((5,)),
            dma,
            dma,
            dma((16,)),
            dma((7,)),
            dma((7,)),
            dma((5,)),
            dma((5,)),
        ],
        compiler_params=pltpu.CompilerParams(collective_id=0, has_side_effects=True),
    )(
        obs_length,
        obs_value.reshape(square),
        obs_frac,
        obs_cell.reshape(square),
        obs_layer.reshape(square),
        obs_tile.reshape(square),
        ensemble.reshape(40, 192, 128),
    )
    return out.reshape(40, 2, 16, 128)


def solution(mesh):
    placed = (
        P(("tx", "ty", "mem")),
        P(None, ("tx", "ty", "mem")),
        P(("tx", "ty", "mem")),
        P(("tx", "ty", "mem")),
        P(("tx", "ty", "mem")),
        P(("tx", "ty", "mem")),
        P("mem", None, None, "tx", "ty"),
    )
    return jax.shard_map(
        body, mesh=mesh, in_specs=placed, out_specs=P("mem", None, "tx", "ty"), check_vma=False
    )
```
